32 devices in a mesh: node: 16 (over z, x, core), col: 2 (over y).
Axes of the slice: x: 2, y: 2, z: 4, core: 2. Of those that a mesh axis runs over, the one named last changes fastest.
Arguments:
- coefficients: bfloat16 [64, 256, 2048], P('node', None, 'col'), may hold values from -6 to 6
- transfer: bfloat16 [3, 64, 4, 256, 256], P(None, 'node', None, 'col'), may hold values from -0.1875 to 0.1875
Outputs:
- result: bfloat16 [64, 256, 2048], P('node', None, 'col')
The draws below stay inside these ranges and needn't reach their ends.
All inputs are finite; a program needn't handle non-finite values.
Results may differ from the reference program's by a relative error of at most 0.0058.
Values may be sent and summed in bfloat16 or wider, within the bound.
A program may use at most 64 MiB of HBM per device.

```python
import jax
import jax.numpy as jnp

RANK = 256
LEVELS = 3
NODES = 64
COLS = 2048


def levels(rng, dims, split, smallest, top_value):
    loudness = 1.0
    for position, shards_of in split:
        draws = jax.random.uniform(jax.random.fold_in(jax.random.fold_in(rng, 6), position), (shards_of,), jnp.float32, smallest / len(split), top_value / len(split))
        loudness = loudness * jnp.repeat(jnp.exp(draws), dims[position] // shards_of).reshape((-1,) + (1,) * (len(dims) - 1 - position))
    return loudness


def bell_draw(stream_key, extent, deviation, bound, shards=(), kind=jnp.bfloat16):
    gain = levels(stream_key, extent, shards, -0.22, 0.18) if shards else 1.0
    entries = jax.random.normal(stream_key, extent, jnp.float32) * deviation * gain
    return jnp.minimum(jnp.maximum(entries, -bound), bound).astype(kind)


def setup_inputs(seed: int = 0) -> dict:
    seeds = jax.random.split(jax.random.key(seed), 3)
    coefficients = bell_draw(seeds[0], (NODES, RANK, COLS), 1.0, 6.0, ((0, 16), (2, 2)))
    transfer = bell_draw(seeds[1], (LEVELS, NODES, 4, RANK, RANK), (4 * RANK) ** -0.5, 0.1875, ((1, 16), (3, 2)))
    return {"coefficients": coefficients, "transfer": transfer}


def reference(coefficients, transfer):
    current = coefficients
    for level_index in range(LEVELS):
        stride = 4 ** level_index
        groups_out = NODES // (4 * stride)
        weights_now = transfer[level_index].reshape(groups_out, 4, stride, 4, RANK, RANK).astype(jnp.float32)
        blocks = current.reshape(groups_out, 4, stride, RANK, COLS).astype(jnp.float32)
        mixed = jnp.einsum('adbjrs,ajbsc->adbrc', weights_now, blocks)
        current = mixed.reshape(NODES, RANK, COLS).astype(jnp.bfloat16)
    return current
```

```python
import functools

import jax
import jax.numpy as jnp
from jax import lax
from jax.experimental import pallas as pl
from jax.experimental.pallas import tpu as pltpu
from jax.sharding import PartitionSpec as P

MESH = pl.DeviceIdType.MESH
WIDTH = 256
LAG_ONE, LAG_RELAY, LAG_FAR, LAG_MID, LAG_END = 3, 5, 8, 11, 13
TO_TWO, FORWARD, TO_PAIR, TO_ACROSS, RELAY, PARTIAL, SUM_NEAR, SUM_FAR = range(8)
ROW = {TO_TWO: 0, FORWARD: 1, TO_PAIR: 2, TO_ACROSS: 3, RELAY: 4, PARTIAL: 3, SUM_NEAR: 3, SUM_FAR: 3}


def flip(i, bit):
    return i + bit - 2 * bit * (i // bit % 2)


def dot(a, b):
    return jnp.dot(a, b, preferred_element_type=jnp.float32)


def kernel(
    cols, chunks, x_in, t_in, out_ref,
    x, t, t_far, t_sum, held, theirs, y1, pair, across, relayed, partial_out, partial_in, sums,
    local_sem, send, recv, t_send, t_recv, far_send, far_recv, sum_send, sum_recv, spread_send, spread_recv,
):
    nodes_here = x_in.shape[0]
    last = nodes_here - 1
    rows = t_in.shape[3]
    units = nodes_here * chunks
    plain = last * chunks
    width = x_in.shape[2] // chunks
    me = lax.axis_index("node")
    my_col = lax.axis_index("col")
    one = me % 4
    two = me // 4 % 4
    side = two // 2 * 2
    other = 2 - side
    is_mid = (two + 1) // 2 % 2 == 1
    is_end = (two + 1) // 2 % 2 == 0
    by_core, by_two, by_pair, by_cross = flip(me, 1), flip(me, 2), flip(me, 4), flip(me, 8)
    by_across = flip(by_pair, 8)
    my_rows = pl.ds(my_col * rows, rows)

    x_copy = pltpu.make_async_copy(x_in, x, local_sem.at[0])
    x_copy.start()
    t_copy = pltpu.make_async_copy(t_in, t.at[:, :, :, my_rows, :], local_sem.at[1])
    t_copy.start()

    barrier = pltpu.get_barrier_semaphore()
    for k in range(1, cols):
        pl.semaphore_signal(barrier, inc=1, device_id={"col": (my_col + k) % cols}, device_id_type=MESH)
    for device in (by_cross, by_pair, by_two, by_core):
        pl.semaphore_signal(barrier, inc=1, device_id={"node": device}, device_id_type=MESH)

    @pl.when(is_mid)
    def _():
        pl.semaphore_signal(barrier, inc=1, device_id={"node": by_across}, device_id_type=MESH)
        pl.semaphore_wait(barrier, 5 + cols - 1)

    @pl.when(is_end)
    def _():
        pl.semaphore_wait(barrier, 4 + cols - 1)

    def remote(source, target, send_sem, recv_sem, device):
        return pltpu.make_async_remote_copy(
            src_ref=source, dst_ref=target, send_sem=send_sem, recv_sem=recv_sem,
            device_id=device, device_id_type=MESH,
        )

    def t_rows(level, m, k, col, children=None):
        here = pl.ds(col * rows, rows)
        if children is None:
            source, target = t_in.at[level, m], t.at[level, m, :, here, :]
        else:
            source, target = t_in.at[level, m, children], t.at[level, m, children, here, :]
        group = 0 if level < 2 else 1 if children is None else 2
        return remote(
            source, target, t_send.at[group, k - 1], t_recv.at[level, m, k - 1], {"col": (my_col + k) % cols}
        )

    def wait_rows(level, m, children=None):
        for k in range(1, cols):
            t_rows(level, m, k, (my_col + cols - k) % cols, children).wait_recv()

    own_side = pl.ds(side, 2)

    order = sorted(
        (2 * m + (0, 1, 3)[level], level, m) for m in range(nodes_here) for level in range(3) if (level, m) != (2, last)
    )
    for _, level, m in order:
        for k in range(1, cols):
            t_rows(level, m, k, my_col).start()

    def t_sum_copy(who, device):
        return remote(
            t_in.at[2, last, pl.ds(other, 2)], t_sum.at[who, :, my_rows, :],
            sum_send.at[0], sum_recv.at[who], {"node": device},
        )

    @pl.when(is_mid)
    def _():
        t_sum_copy(0, by_across).start()

    @pl.when(is_end)
    def _():
        t_sum_copy(1, by_cross).start()

    def spread(k, col):
        part = t_sum.at[:, :, pl.ds(col * rows, rows), :]
        return remote(part, part, spread_send.at[k - 1], spread_recv.at[k - 1], {"col": (my_col + k) % cols})

    def copy(kind, u):
        source, target, device = {
            TO_TWO: lambda: (held.at[u, 0], held.at[u, 1], by_two),
            FORWARD: lambda: (held.at[u], theirs.at[u], by_core),
            TO_PAIR: lambda: (y1.at[u], pair.at[u], by_pair),
            TO_ACROSS: lambda: (y1.at[u], across.at[u], by_across),
            RELAY: lambda: (pair.at[u], relayed.at[u], by_across),
            PARTIAL: lambda: (partial_out.at[u], partial_in.at[u], by_pair),
            SUM_NEAR: lambda: (sums.at[0, u - plain], across.at[u], by_across),
            SUM_FAR: lambda: (sums.at[1, u - plain], partial_in.at[u], by_cross),
        }[kind]()
        return remote(source, target, send.at[kind], recv.at[ROW[kind], u], {"node": device})

    def sent(kind, source, target):
        remote(source, target, send.at[kind], recv.at[ROW[kind], 0], {"node": by_pair}).wait_send()

    def far(m):
        return remote(
            t.at[2, m, pl.ds(1 - two // 3, 3)], t_far.at[m], far_send.at[0], far_recv.at[m], {"node": by_pair}
        )

    def store(u, total):
        columns = pl.ds(pl.multiple_of(u % chunks * width, width), width)
        out_ref[u // chunks, :, columns] = total.astype(out_ref.dtype)

    def first(u, action):
        @pl.when(u % chunks == 0)
        def _():
            action(u // chunks)

    def stage_zero(u):
        first(u, lambda m: wait_rows(0, m))
        m = u // chunks
        columns = pl.ds(pl.multiple_of(u % chunks * width, width), width)
        total = dot(t[0, m, 0], x[0, :, columns])
        for j in range(1, 4):
            total += dot(t[0, m, j], x[j, :, columns])
        held[u, 0] = total.astype(held.dtype)
        copy(TO_TWO, u).start()

    def stage_one(u):
        copy(TO_TWO, u).wait_recv()
        copy(FORWARD, u).start()
        first(u, lambda m: wait_rows(1, m))
        m = u // chunks
        total = dot(t[1, m, one], held[u, 0])
        total += dot(t[1, m, flip(one, 2)], held[u, 1])
        copy(FORWARD, u).wait_recv()
        total += dot(t[1, m, flip(one, 1)], theirs[u, 0])
        total += dot(t[1, m, 3 - one], theirs[u, 1])
        y1[u] = total.astype(y1.dtype)

        @pl.when(is_mid & (u < plain))
        def _():
            copy(TO_ACROSS, u).start()

        @pl.when(is_end | (u >= plain))
        def _():
            copy(TO_PAIR, u).start()

    def stage_relay(u):
        copy(TO_PAIR, u).wait_recv()

        @pl.when(u < plain)
        def _():
            copy(RELAY, u).start()

        @pl.when(u >= plain)
        def _():
            @pl.when(u == plain)
            def _():
                for k in range(1, cols):
                    spread(k, (my_col + cols - k) % cols).wait_recv()

            for who, kind in ((1, SUM_FAR), (0, SUM_NEAR)):
                total = dot(t_sum[who, two % 2], y1[u]) + dot(t_sum[who, 1 - two % 2], pair[u])
                sums[who, u - plain] = total.astype(sums.dtype)
                copy(kind, u).start()

    def stage_far(u):
        def send_far(m):
            wait_rows(2, m)
            far(m).start()

        @pl.when(u < plain)
        def _():
            first(u, send_far)

    def own_part(u):
        m = u // chunks
        return dot(t[2, m, two], y1[u])

    def pair_part(u):
        return dot(t[2, u // chunks, flip(two, 1)], pair[u])

    def stage_mid(u):
        @pl.when(u < plain)
        def _():
            def arrive(m):
                wait_rows(2, m)
                far(m).wait_recv()

            first(u, arrive)
            m = u // chunks
            copy(TO_ACROSS, u).wait_recv()
            copy(RELAY, u).wait_recv()
            start = 1 - two // 2
            part = dot(t_far[m, 3 - two - start], across[u])
            part += dot(t_far[m, flip(3 - two, 1) - start], relayed[u])
            part += dot(t_far[m, two - start], y1[u])
            partial_out[u] = part.astype(partial_out.dtype)
            copy(PARTIAL, u).start()
            total = own_part(u) + pair_part(u)
            total += dot(t[2, m, 3 - two], across[u])
            total += dot(t[2, m, flip(two, 2)], relayed[u])
            store(u, total)

        @pl.when(u >= plain)
        def _():
            @pl.when(u == plain)
            def _():
                wait_rows(2, last, own_side)

            total = own_part(u) + pair_part(u)
            copy(SUM_NEAR, u).wait_recv()
            store(u, total + across[u].astype(jnp.float32))

    def stage_end(u):
        @pl.when(u < plain)
        def _():
            total = own_part(u)
            copy(PARTIAL, u).wait_recv()
            store(u, total + partial_in[u].astype(jnp.float32))

        @pl.when(u >= plain)
        def _():
            @pl.when(u == plain)
            def _():
                wait_rows(2, last, own_side)

            copy(TO_PAIR, u).wait_recv()
            total = own_part(u) + pair_part(u)
            copy(SUM_FAR, u).wait_recv()
            store(u, total + partial_in[u].astype(jnp.float32))

    x_copy.wait()
    t_copy.wait()

    def step(s, _):
        def run(stage, lag, role=None):
            u = s - lag
            ready = (u >= 0) & (u < units)

            @pl.when(ready if role is None else ready & role)
            def _():
                stage(u)

        run(stage_one, LAG_ONE)

        @pl.when(s == LAG_ONE)
        def _():
            @pl.when(is_mid)
            def _():
                for who, device in enumerate((by_across, by_cross)):
                    t_sum_copy(who, device).wait_recv()
                for k in range(1, cols):
                    spread(k, my_col).start()

            for k in range(1, cols):
                t_rows(2, last, k, my_col, own_side).start()

        run(stage_relay, LAG_RELAY, is_mid)
        run(stage_far, LAG_FAR, is_end)
        run(stage_mid, LAG_MID, is_mid)
        run(stage_end, LAG_END, is_end)
        run(stage_zero, 0)
        return 0

    lax.fori_loop(0, units + LAG_END, step, 0)

    sent(TO_TWO, held.at[:, 0], held.at[:, 1])
    sent(FORWARD, held, theirs)

    @pl.when(is_mid)
    def _():
        early = pl.ds(0, plain)
        late = pl.ds(plain, units - plain)
        sent(TO_PAIR, y1.at[late], pair.at[late])
        sent(TO_ACROSS, y1.at[early], across.at[early])
        sent(RELAY, pair.at[early], relayed)
        sent(PARTIAL, partial_out, partial_in.at[early])
        sent(SUM_NEAR, sums.at[0], across.at[late])
        sent(SUM_FAR, sums.at[1], across.at[late])
        for k in range(1, cols):
            spread(k, my_col).wait_send()

    @pl.when(is_end)
    def _():
        sent(TO_PAIR, y1, pair)
        remote(t_far, t_far, far_send.at[0], far_recv.at[0], {"node": by_pair}).wait_send()

    t_sum_copy(0, by_across).wait_send()
    for k in range(1, cols):
        beside = {"col": (my_col + k) % cols}
        both, rest = t_in.at[pl.ds(0, 2)], t_in.at[2, pl.ds(0, last)]
        remote(both, t.at[pl.ds(0, 2), :, :, my_rows, :], t_send.at[0, k - 1], t_recv.at[0, 0, k - 1], beside).wait_send()
        remote(
            rest, t.at[2, pl.ds(0, last), :, my_rows, :], t_send.at[1, k - 1], t_recv.at[0, 0, k - 1], beside
        ).wait_send()
        t_rows(2, last, k, my_col, own_side).wait_send()


def local(coefficients, transfer):
    cols = lax.axis_size("col")
    nodes_here, rank, columns = coefficients.shape
    levels, _, children, rows, _ = transfer.shape
    width = min(WIDTH, columns)
    chunks = columns // width
    units = nodes_here * chunks
    plain = units - chunks
    others = max(cols - 1, 1)
    kind = coefficients.dtype
    block = (rank, width)
    dma = pltpu.SemaphoreType.DMA
    return pl.pallas_call(
        functools.partial(kernel, cols, chunks),
        out_shape=pltpu.VMEM(coefficients.shape, kind),
        in_specs=[pl.BlockSpec(memory_space=pl.ANY)] * 2,
        out_specs=pl.BlockSpec(memory_space=pltpu.VMEM),
        scratch_shapes=[
            pltpu.VMEM(coefficients.shape, kind),
            pltpu.VMEM((levels, nodes_here, children, rank, rank), kind),
            pltpu.VMEM((nodes_here - 1, children - 1, rank, rank), kind),
            pltpu.VMEM((2, 2, rank, rank), kind),
            pltpu.VMEM((units, 2) + block, kind),
            pltpu.VMEM((units, 2) + block, kind),
            pltpu.VMEM((units,) + block, kind),
            pltpu.VMEM((units,) + block, kind),
            pltpu.VMEM((units,) + block, kind),
            pltpu.VMEM((plain,) + block, kind),
            pltpu.VMEM((plain,) + block, kind),
            pltpu.VMEM((units,) + block, kind),
            pltpu.VMEM((2, chunks) + block, kind),
            dma((2,)),
            dma((8,)),
            dma((5, units)),
            dma((3, others)),
            dma((levels, nodes_here, others)),
            dma((1,)),
            dma((nodes_here - 1,)),
            dma((1,)),
            dma((2,)),
            dma((others,)),
            dma((others,)),
        ],
        compiler_params=pltpu.CompilerParams(
            collective_id=0, has_side_effects=True, vmem_limit_bytes=56 * 1024 * 1024
        ),
    )(coefficients, transfer)


def solution(mesh):
    return jax.shard_map(
        local,
        mesh=mesh,
        in_specs=(P("node", None, "col"), P(None, "node", None, "col", None)),
        out_specs=P("node", None, "col"),
        check_vma=False,
    )
```

```python
import functools

import jax
import jax.numpy as jnp
from jax import lax
from jax.experimental import pallas as pl
from jax.experimental.pallas import tpu as pltpu
from jax.sharding import PartitionSpec as P

MESH = pl.DeviceIdType.MESH
WIDTH = 256
HELD_BACK = 2
LAG_ONE, LAG_RELAY, LAG_FAR, LAG_MID, LAG_NEAR, LAG_END = 2, 4, 5, 7, 8, 10
TO_TWO, FORWARD, TO_PAIR, TO_ACROSS, RELAY, PARTIAL, SUM_NEAR, SUM_FAR = range(8)
ROW = {TO_TWO: 0, FORWARD: 1, TO_PAIR: 2, TO_ACROSS: 3, RELAY: 4, PARTIAL: 3, SUM_NEAR: 3, SUM_FAR: 4}


def flip(i, bit):
    return i + bit - 2 * bit * (i // bit % 2)


def dot(a, b):
    return jnp.dot(a, b, preferred_element_type=jnp.float32)


def kernel(
    cols, chunks, x_in, t_in, out_ref,
    x, t, t_far, t_pass, t_sum, held, theirs, y1, pair, across, relayed, partial_out, partial_in, sums,
    local_sem, send, recv, t_send, t_recv, far_send, far_recv, sum_send, sum_recv, spread_send, spread_recv,
):
    nodes_here = x_in.shape[0]
    last = nodes_here - 1
    rows = t_in.shape[3]
    units = nodes_here * chunks
    plain = last * chunks
    width = x_in.shape[2] // chunks
    me = lax.axis_index("node")
    my_col = lax.axis_index("col")
    one = me % 4
    two = me // 4 % 4
    side = two // 2 * 2
    other = 2 - side
    is_mid = (two + 1) // 2 % 2 == 1
    is_end = (two + 1) // 2 % 2 == 0
    by_core, by_two, by_pair = flip(me, 1), flip(me, 2), flip(me, 4)
    by_across = flip(by_pair, 8)
    my_rows = pl.ds(my_col * rows, rows)

    x_copy = pltpu.make_async_copy(x_in, x, local_sem.at[0])
    x_copy.start()
    t_copy = pltpu.make_async_copy(t_in, t.at[:, :, :, my_rows, :], local_sem.at[1])
    t_copy.start()

    barrier = pltpu.get_barrier_semaphore()
    for k in range(1, cols):
        pl.semaphore_signal(barrier, inc=1, device_id={"col": (my_col + k) % cols}, device_id_type=MESH)
    for device in (by_pair, by_two, by_core):
        pl.semaphore_signal(barrier, inc=1, device_id={"node": device}, device_id_type=MESH)

    @pl.when(is_mid)
    def _():
        pl.semaphore_signal(barrier, inc=1, device_id={"node": by_across}, device_id_type=MESH)
        pl.semaphore_wait(barrier, 4 + cols - 1)

    @pl.when(is_end)
    def _():
        pl.semaphore_wait(barrier, 3 + cols - 1)

    def remote(source, target, send_sem, recv_sem, device):
        return pltpu.make_async_remote_copy(
            src_ref=source, dst_ref=target, send_sem=send_sem, recv_sem=recv_sem,
            device_id=device, device_id_type=MESH,
        )

    def t_rows(level, m, k, col, children=None):
        here = pl.ds(col * rows, rows)
        if children is None:
            source, target = t_in.at[level, m], t.at[level, m, :, here, :]
        else:
            source, target = t_in.at[level, m, children], t.at[level, m, children, here, :]
        group = 0 if level < 2 else 1 if children is None else 2
        return remote(
            source, target, t_send.at[group, k - 1], t_recv.at[level, m, k - 1], {"col": (my_col + k) % cols}
        )

    def wait_rows(level, m, children=None):
        for k in range(1, cols):
            t_rows(level, m, k, (my_col + cols - k) % cols, children).wait_recv()

    own_side = pl.ds(side, 2)

    order = sorted(
        (3 * m + 2 * level, level, m) for m in range(nodes_here) for level in range(3) if (level, m) != (2, last)
    )
    for _, level, m in order:
        for k in range(1, cols):
            t_rows(level, m, k, my_col).start()

    given = t_in.at[2, last, pl.ds(other, 2)]

    def give():
        return remote(given, t_sum.at[0, :, my_rows, :], sum_send.at[0], sum_recv.at[0], {"node": by_across})

    def give_pair():
        return remote(given, t_pass, sum_send.at[0], sum_recv.at[2], {"node": by_pair})

    def give_on():
        return remote(t_pass, t_sum.at[1, :, my_rows, :], sum_send.at[1], sum_recv.at[1], {"node": by_across})

    @pl.when(is_mid)
    def _():
        give().start()

    @pl.when(is_end)
    def _():
        give_pair().start()

    def spread(k, col):
        part = t_sum.at[:, :, pl.ds(col * rows, rows), :]
        return remote(part, part, spread_send.at[k - 1], spread_recv.at[k - 1], {"col": (my_col + k) % cols})

    def copy(kind, u):
        source, target, device = {
            TO_TWO: lambda: (held.at[u, 0], held.at[u, 1], by_two),
            FORWARD: lambda: (held.at[u], theirs.at[u], by_core),
            TO_PAIR: lambda: (y1.at[u], pair.at[u], by_pair),
            TO_ACROSS: lambda: (y1.at[u], across.at[u], by_across),
            RELAY: lambda: (pair.at[u], relayed.at[u], by_across),
            PARTIAL: lambda: (partial_out.at[u], partial_in.at[u], by_pair),
            SUM_NEAR: lambda: (sums.at[0, u - plain], across.at[u], by_across),
            SUM_FAR: lambda: (sums.at[1, u - plain], relayed.at[u], by_across),
        }[kind]()
        return remote(source, target, send.at[kind], recv.at[ROW[kind], u], {"node": device})

    def sent(kind, source, target):
        remote(source, target, send.at[kind], recv.at[ROW[kind], 0], {"node": by_pair}).wait_send()

    def far(m):
        if isinstance(m, int) and m == last:
            source, target, sem = t.at[2, m, flip(two, 1)], t_far.at[m, 0], far_send.at[1]
        else:
            source, target, sem = t.at[2, m, pl.ds(1 - two // 3, 3)], t_far.at[m], far_send.at[0]
        return remote(source, target, sem, far_recv.at[m], {"node": by_pair})

    def store(u, total):
        columns = pl.ds(pl.multiple_of(u % chunks * width, width), width)
        out_ref[u // chunks, :, columns] = total.astype(out_ref.dtype)

    def first(u, action):
        @pl.when(u % chunks == 0)
        def _():
            action(u // chunks)

    def zero_rows(u, here):
        columns = pl.ds(pl.multiple_of(u % chunks * width, width), width)
        total = dot(t[0, 0, 0, here], x[0, :, columns])
        for j in range(1, 4):
            total += dot(t[0, 0, j, here], x[j, :, columns])
        held[u, 0, here] = total.astype(held.dtype)
        remote(
            held.at[u, 0, here], held.at[u, 1, here], send.at[TO_TWO], recv.at[ROW[TO_TWO], u], {"node": by_two}
        ).start()

    def own_rows(u, _):
        zero_rows(u, pl.ds(pl.multiple_of(my_col * rows, rows), rows))
        return 0

    def stage_zero(u):
        first(u, lambda m: wait_rows(0, m))

        @pl.when(u < chunks)
        def _():
            for k in range(1, cols):
                zero_rows(u, pl.ds(pl.multiple_of((my_col + k) % cols * rows, rows), rows))

        @pl.when(u >= chunks)
        def _():
            m = u // chunks
            columns = pl.ds(pl.multiple_of(u % chunks * width, width), width)
            total = dot(t[0, m, 0], x[0, :, columns])
            for j in range(1, 4):
                total += dot(t[0, m, j], x[j, :, columns])
            held[u, 0] = total.astype(held.dtype)
            copy(TO_TWO, u).start()

    def stage_one(u):
        copy(TO_TWO, u).wait_recv()
        copy(FORWARD, u).start()
        first(u, lambda m: wait_rows(1, m))
        m = u // chunks
        total = dot(t[1, m, one], held[u, 0])
        total += dot(t[1, m, flip(one, 2)], held[u, 1])
        copy(FORWARD, u).wait_recv()
        total += dot(t[1, m, flip(one, 1)], theirs[u, 0])
        total += dot(t[1, m, 3 - one], theirs[u, 1])
        y1[u] = total.astype(y1.dtype)

        @pl.when(is_mid & (u < plain))
        def _():
            copy(TO_ACROSS, u).start()

        @pl.when(is_end)
        def _():
            copy(TO_PAIR, u).start()

    def stage_relay(u):
        copy(TO_PAIR, u).wait_recv()

        @pl.when(u < plain)
        def _():
            copy(RELAY, u).start()

        @pl.when(u >= plain)
        def _():
            @pl.when(u == plain)
            def _():
                for k in range(1, cols):
                    spread(k, (my_col + cols - k) % cols).wait_recv()

            for who, kind in ((1, SUM_FAR), (0, SUM_NEAR)):
                total = dot(t_sum[who, two % 2], y1[u]) + dot(t_sum[who, 1 - two % 2], pair[u])
                sums[who, u - plain] = total.astype(sums.dtype)
                if kind == SUM_FAR:
                    copy(kind, u).start()

            @pl.when(u < units - HELD_BACK)
            def _():
                copy(SUM_NEAR, u).start()

            @pl.when(u == units - 1)
            def _():
                for late in range(min(HELD_BACK, chunks), 0, -1):
                    copy(SUM_NEAR, units - late).start()

    def stage_far(m):
        wait_rows(2, m, own_side if m == last else None)
        far(m).start()

    def own_part(u):
        m = u // chunks
        return dot(t[2, m, two], y1[u])

    def pair_part(u):
        return dot(t[2, u // chunks, flip(two, 1)], pair[u])

    def stage_mid(u):
        @pl.when(u < plain)
        def _():
            def arrive(m):
                wait_rows(2, m)
                far(m).wait_recv()

            first(u, arrive)
            m = u // chunks
            copy(TO_ACROSS, u).wait_recv()
            copy(RELAY, u).wait_recv()
            start = 1 - two // 2
            part = dot(t_far[m, 3 - two - start], across[u])
            part += dot(t_far[m, flip(3 - two, 1) - start], relayed[u])
            part += dot(t_far[m, two - start], y1[u])
            partial_out[u] = part.astype(partial_out.dtype)
            copy(PARTIAL, u).start()
            total = own_part(u) + pair_part(u)
            total += dot(t[2, m, 3 - two], across[u])
            total += dot(t[2, m, flip(two, 2)], relayed[u])
            store(u, total)

        @pl.when(u >= plain)
        def _():
            @pl.when(u == plain)
            def _():
                wait_rows(2, last, own_side)
                far(last).wait_recv()

            copy(SUM_FAR, u).wait_recv()
            part = dot(t_far[last, 0], y1[u]) + relayed[u].astype(jnp.float32)
            partial_out[u] = part.astype(partial_out.dtype)
            copy(PARTIAL, u).start()

    def stage_near(u):
        @pl.when(u >= plain)
        def _():
            total = own_part(u) + pair_part(u)
            copy(SUM_NEAR, u).wait_recv()
            store(u, total + across[u].astype(jnp.float32))

    def stage_end(u):
        total = own_part(u)
        copy(PARTIAL, u).wait_recv()
        store(u, total + partial_in[u].astype(jnp.float32))

    x_copy.wait()
    t_copy.wait()
    lax.fori_loop(0, chunks, own_rows, 0)

    @pl.when(is_mid)
    def _():
        give_pair().wait_recv()
        give_on().start()

    def step(s, _):
        def run(stage, lag, role=None):
            u = s - lag
            ready = (u >= 0) & (u < units)

            @pl.when(ready if role is None else ready & role)
            def _():
                stage(u)

        run(stage_relay, LAG_RELAY, is_mid)
        run(stage_one, LAG_ONE)

        @pl.when(s == LAG_ONE)
        def _():
            @pl.when(is_mid)
            def _():
                give().wait_recv()
                give_on().wait_recv()
                for k in range(1, cols):
                    spread(k, my_col).start()

            for k in range(1, cols):
                t_rows(2, last, k, my_col, own_side).start()

        run(stage_zero, 0)
        for m in range(nodes_here):

            @pl.when(is_end & (s == LAG_FAR + m * chunks))
            def _(m=m):
                stage_far(m)

        run(stage_mid, LAG_MID, is_mid)
        run(stage_near, LAG_NEAR, is_mid)
        run(stage_end, LAG_END, is_end)
        return 0

    lax.fori_loop(0, units + LAG_END, step, 0)

    sent(TO_TWO, held.at[:, 0], held.at[:, 1])
    sent(FORWARD, held, theirs)

    @pl.when(is_mid)
    def _():
        early = pl.ds(0, plain)
        late = pl.ds(plain, units - plain)
        sent(TO_ACROSS, y1.at[early], across.at[early])
        sent(RELAY, pair.at[early], relayed.at[early])
        sent(PARTIAL, partial_out, partial_in)
        sent(SUM_NEAR, sums.at[0], across.at[late])
        sent(SUM_FAR, sums.at[1], across.at[late])
        give().wait_send()
        give_on().wait_send()
        for k in range(1, cols):
            spread(k, my_col).wait_send()

    @pl.when(is_end)
    def _():
        sent(TO_PAIR, y1, pair)
        whole = t_far.at[pl.ds(0, last)]
        remote(whole, whole, far_send.at[0], far_recv.at[0], {"node": by_pair}).wait_send()
        far(last).wait_send()
        give_pair().wait_send()

    for k in range(1, cols):
        beside = {"col": (my_col + k) % cols}
        both, rest = t_in.at[pl.ds(0, 2)], t_in.at[2, pl.ds(0, last)]
        remote(both, t.at[pl.ds(0, 2), :, :, my_rows, :], t_send.at[0, k - 1], t_recv.at[0, 0, k - 1], beside).wait_send()
        remote(
            rest, t.at[2, pl.ds(0, last), :, my_rows, :], t_send.at[1, k - 1], t_recv.at[0, 0, k - 1], beside
        ).wait_send()
        t_rows(2, last, k, my_col, own_side).wait_send()


def local(coefficients, transfer):
    cols = lax.axis_size("col")
    nodes_here, rank, columns = coefficients.shape
    levels, _, children, rows, _ = transfer.shape
    width = min(WIDTH, columns)
    chunks = columns // width
    units = nodes_here * chunks
    plain = units - chunks
    others = max(cols - 1, 1)
    kind = coefficients.dtype
    block = (rank, width)
    dma = pltpu.SemaphoreType.DMA
    return pl.pallas_call(
        functools.partial(kernel, cols, chunks),
        out_shape=pltpu.VMEM(coefficients.shape, kind),
        in_specs=[pl.BlockSpec(memory_space=pl.ANY)] * 2,
        out_specs=pl.BlockSpec(memory_space=pltpu.VMEM),
        scratch_shapes=[
            pltpu.VMEM(coefficients.shape, kind),
            pltpu.VMEM((levels, nodes_here, children, rank, rank), kind),
            pltpu.VMEM((nodes_here, children - 1, rank, rank), kind),
            pltpu.VMEM((2, rows, rank), kind),
            pltpu.VMEM((2, 2, rank, rank), kind),
            pltpu.VMEM((units, 2) + block, kind),
            pltpu.VMEM((units, 2) + block, kind),
            pltpu.VMEM((units,) + block, kind),
            pltpu.VMEM((units,) + block, kind),
            pltpu.VMEM((units,) + block, kind),
            pltpu.VMEM((units,) + block, kind),
            pltpu.VMEM((units,) + block, kind),
            pltpu.VMEM((units,) + block, kind),
            pltpu.VMEM((2, chunks) + block, kind),
            dma((2,)),
            dma((8,)),
            dma((5, units)),
            dma((3, others)),
            dma((levels, nodes_here, others)),
            dma((2,)),
            dma((nodes_here,)),
            dma((2,)),
            dma((3,)),
            dma((others,)),
            dma((others,)),
        ],
        compiler_params=pltpu.CompilerParams(
            collective_id=0, has_side_effects=True, vmem_limit_bytes=56 * 1024 * 1024
        ),
    )(coefficients, transfer)


def solution(mesh):
    return jax.shard_map(
        local,
        mesh=mesh,
        in_specs=(P("node", None, "col"), P(None, "node", None, "col", None)),
        out_specs=P("node", None, "col"),
        check_vma=False,
    )
```

```python
import functools

import jax
import jax.numpy as jnp
from jax import lax
from jax.experimental import pallas as pl
from jax.experimental.pallas import tpu as pltpu
from jax.sharding import PartitionSpec as P

MESH = pl.DeviceIdType.MESH
WIDTH = 256
HELD_BACK = 3
LAG_ONE, LAG_RELAY, LAG_FAR, LAG_MID, LAG_NEAR, LAG_END = 2, 5, 4, 9, 13, 12
TO_TWO, FORWARD, TO_PAIR, TO_ACROSS, RELAY, PARTIAL, SUM_NEAR, SUM_FAR = range(8)
ROW = {TO_TWO: 0, FORWARD: 1, TO_PAIR: 2, TO_ACROSS: 3, RELAY: 4, PARTIAL: 3, SUM_NEAR: 3, SUM_FAR: 4}


def flip(i, bit):
    return i + bit - 2 * bit * (i // bit % 2)


def dot(a, b):
    return jnp.dot(a, b, preferred_element_type=jnp.float32)


def kernel(
    cols, chunks, x_in, t_in, out_ref,
    x, t, t_far, t_pass, t_sum, held, theirs, y1, pair, across, relayed, partial_out, partial_in, sums,
    local_sem, send, recv, t_send, t_recv, far_send, far_recv, sum_send, sum_recv, spread_send, spread_recv,
):
    nodes_here = x_in.shape[0]
    last = nodes_here - 1
    rows = t_in.shape[3]
    units = nodes_here * chunks
    plain = last * chunks
    width = x_in.shape[2] // chunks
    me = lax.axis_index("node")
    my_col = lax.axis_index("col")
    one = me % 4
    two = me // 4 % 4
    side = two // 2 * 2
    other = 2 - side
    is_mid = (two + 1) // 2 % 2 == 1
    is_end = (two + 1) // 2 % 2 == 0
    by_core, by_two, by_pair = flip(me, 1), flip(me, 2), flip(me, 4)
    by_across = flip(by_pair, 8)
    my_rows = pl.ds(my_col * rows, rows)

    x_copy = pltpu.make_async_copy(x_in, x, local_sem.at[0])
    x_copy.start()
    t_copy = pltpu.make_async_copy(t_in, t.at[:, :, :, my_rows, :], local_sem.at[1])
    t_copy.start()

    barrier = pltpu.get_barrier_semaphore()
    for k in range(1, cols):
        pl.semaphore_signal(barrier, inc=1, device_id={"col": (my_col + k) % cols}, device_id_type=MESH)
    for device in (by_pair, by_two, by_core):
        pl.semaphore_signal(barrier, inc=1, device_id={"node": device}, device_id_type=MESH)

    @pl.when(is_mid)
    def _():
        pl.semaphore_signal(barrier, inc=1, device_id={"node": by_across}, device_id_type=MESH)
        pl.semaphore_wait(barrier, 4 + cols - 1)

    @pl.when(is_end)
    def _():
        pl.semaphore_wait(barrier, 3 + cols - 1)

    def remote(source, target, send_sem, recv_sem, device):
        return pltpu.make_async_remote_copy(
            src_ref=source, dst_ref=target, send_sem=send_sem, recv_sem=recv_sem,
            device_id=device, device_id_type=MESH,
        )

    def t_rows(level, m, k, col, children=None):
        here = pl.ds(col * rows, rows)
        if children is None:
            source, target = t_in.at[level, m], t.at[level, m, :, here, :]
        else:
            source, target = t_in.at[level, m, children], t.at[level, m, children, here, :]
        group = 0 if level < 2 else 1 if children is None else 2
        return remote(
            source, target, t_send.at[group, k - 1], t_recv.at[level, m, k - 1], {"col": (my_col + k) % cols}
        )

    def wait_rows(level, m, children=None):
        for k in range(1, cols):
            t_rows(level, m, k, (my_col + cols - k) % cols, children).wait_recv()

    own_side = pl.ds(side, 2)

    order = sorted(
        (3 * m + 2 * level, level, m) for m in range(nodes_here) for level in range(3) if (level, m) != (2, last)
    )
    for _, level, m in order:
        for k in range(1, cols):
            t_rows(level, m, k, my_col).start()

    given = t_in.at[2, last, pl.ds(other, 2)]

    def give():
        return remote(given, t_sum.at[0, :, my_rows, :], sum_send.at[0], sum_recv.at[0], {"node": by_across})

    def give_pair():
        return remote(given, t_pass, sum_send.at[0], sum_recv.at[2], {"node": by_pair})

    def give_on():
        return remote(t_pass, t_sum.at[1, :, my_rows, :], sum_send.at[1], sum_recv.at[1], {"node": by_across})

    @pl.when(is_mid)
    def _():
        give().start()

    @pl.when(is_end)
    def _():
        give_pair().start()

    def spread(k, col):
        part = t_sum.at[:, :, pl.ds(col * rows, rows), :]
        return remote(part, part, spread_send.at[k - 1], spread_recv.at[k - 1], {"col": (my_col + k) % cols})

    def copy(kind, u):
        source, target, device = {
            TO_TWO: lambda: (held.at[u, 0], held.at[u, 1], by_two),
            FORWARD: lambda: (held.at[u], theirs.at[u], by_core),
            TO_PAIR: lambda: (y1.at[u], pair.at[u], by_pair),
            TO_ACROSS: lambda: (y1.at[u], across.at[u], by_across),
            RELAY: lambda: (pair.at[u], relayed.at[u], by_across),
            PARTIAL: lambda: (partial_out.at[u], partial_in.at[u], by_pair),
            SUM_NEAR: lambda: (sums.at[0, u - plain], across.at[u], by_across),
            SUM_FAR: lambda: (sums.at[1, u - plain], relayed.at[u], by_across),
        }[kind]()
        return remote(source, target, send.at[kind], recv.at[ROW[kind], u], {"node": device})

    def sent(kind, source, target):
        remote(source, target, send.at[kind], recv.at[ROW[kind], 0], {"node": by_pair}).wait_send()

    def far(m):
        if isinstance(m, int) and m == last:
            source, target, sem = t.at[2, m, flip(two, 1)], t_far.at[m, 0], far_send.at[1]
        else:
            source, target, sem = t.at[2, m, pl.ds(1 - two // 3, 3)], t_far.at[m], far_send.at[0]
        return remote(source, target, sem, far_recv.at[m], {"node": by_pair})

    def store(u, total):
        columns = pl.ds(pl.multiple_of(u % chunks * width, width), width)
        out_ref[u // chunks, :, columns] = total.astype(out_ref.dtype)

    def first(u, action):
        @pl.when(u % chunks == 0)
        def _():
            action(u // chunks)

    def zero_rows(u, here):
        columns = pl.ds(pl.multiple_of(u % chunks * width, width), width)
        total = dot(t[0, 0, 0, here], x[0, :, columns])
        for j in range(1, 4):
            total += dot(t[0, 0, j, here], x[j, :, columns])
        held[u, 0, here] = total.astype(held.dtype)
        remote(
            held.at[u, 0, here], held.at[u, 1, here], send.at[TO_TWO], recv.at[ROW[TO_TWO], u], {"node": by_two}
        ).start()

    def own_rows(u, _):
        zero_rows(u, pl.ds(pl.multiple_of(my_col * rows, rows), rows))
        return 0

    def stage_zero(u):
        first(u, lambda m: wait_rows(0, m))

        @pl.when(u < chunks)
        def _():
            for k in range(1, cols):
                zero_rows(u, pl.ds(pl.multiple_of((my_col + k) % cols * rows, rows), rows))

        @pl.when(u >= chunks)
        def _():
            m = u // chunks
            columns = pl.ds(pl.multiple_of(u % chunks * width, width), width)
            total = dot(t[0, m, 0], x[0, :, columns])
            for j in range(1, 4):
                total += dot(t[0, m, j], x[j, :, columns])
            held[u, 0] = total.astype(held.dtype)
            copy(TO_TWO, u).start()

    def stage_one(u):
        copy(TO_TWO, u).wait_recv()
        copy(FORWARD, u).start()
        first(u, lambda m: wait_rows(1, m))
        m = u // chunks
        total = dot(t[1, m, one], held[u, 0])
        total += dot(t[1, m, flip(one, 2)], held[u, 1])
        copy(FORWARD, u).wait_recv()
        total += dot(t[1, m, flip(one, 1)], theirs[u, 0])
        total += dot(t[1, m, 3 - one], theirs[u, 1])
        y1[u] = total.astype(y1.dtype)

        @pl.when(is_mid & (u < plain))
        def _():
            copy(TO_ACROSS, u).start()

        @pl.when(is_end)
        def _():
            copy(TO_PAIR, u).start()

    def stage_relay(u):
        copy(TO_PAIR, u).wait_recv()

        @pl.when(u < plain)
        def _():
            copy(RELAY, u).start()

        @pl.when(u >= plain)
        def _():
            @pl.when(u == plain)
            def _():
                for k in range(1, cols):
                    spread(k, (my_col + cols - k) % cols).wait_recv()

            for who, kind in ((1, SUM_FAR), (0, SUM_NEAR)):
                total = dot(t_sum[who, two % 2], y1[u]) + dot(t_sum[who, 1 - two % 2], pair[u])
                sums[who, u - plain] = total.astype(sums.dtype)
                if kind == SUM_FAR:
                    copy(kind, u).start()

            @pl.when(u < units - HELD_BACK)
            def _():
                copy(SUM_NEAR, u).start()

            @pl.when(u == units - 1)
            def _():
                for late in range(min(HELD_BACK, chunks), 0, -1):
                    copy(SUM_NEAR, units - late).start()

    def stage_far(m):
        wait_rows(2, m, own_side if m == last else None)
        far(m).start()

    def own_part(u):
        m = u // chunks
        return dot(t[2, m, two], y1[u])

    def pair_part(u):
        return dot(t[2, u // chunks, flip(two, 1)], pair[u])

    def stage_mid(u):
        @pl.when(u < plain)
        def _():
            def arrive(m):
                wait_rows(2, m)
                far(m).wait_recv()

            first(u, arrive)
            m = u // chunks
            copy(TO_ACROSS, u).wait_recv()
            copy(RELAY, u).wait_recv()
            start = 1 - two // 2
            part = dot(t_far[m, 3 - two - start], across[u])
            part += dot(t_far[m, flip(3 - two, 1) - start], relayed[u])
            part += dot(t_far[m, two - start], y1[u])
            partial_out[u] = part.astype(partial_out.dtype)
            copy(PARTIAL, u).start()
            total = own_part(u) + pair_part(u)
            total += dot(t[2, m, 3 - two], across[u])
            total += dot(t[2, m, flip(two, 2)], relayed[u])
            store(u, total)

        @pl.when(u >= plain)
        def _():
            @pl.when(u == plain)
            def _():
                wait_rows(2, last, own_side)
                far(last).wait_recv()

            copy(SUM_FAR, u).wait_recv()
            part = dot(t_far[last, 0], y1[u]) + relayed[u].astype(jnp.float32)
            partial_out[u] = part.astype(partial_out.dtype)
            copy(PARTIAL, u).start()

    def stage_near(u):
        @pl.when(u >= plain)
        def _():
            total = own_part(u) + pair_part(u)
            copy(SUM_NEAR, u).wait_recv()
            store(u, total + across[u].astype(jnp.float32))

    def stage_end(u):
        total = own_part(u)
        copy(PARTIAL, u).wait_recv()
        store(u, total + partial_in[u].astype(jnp.float32))

    x_copy.wait()
    t_copy.wait()
    lax.fori_loop(0, chunks, own_rows, 0)

    @pl.when(is_mid)
    def _():
        give_pair().wait_recv()
        give_on().start()

    def step(s, _):
        def run(stage, lag, role=None):
            u = s - lag
            ready = (u >= 0) & (u < units)

            @pl.when(ready if role is None else ready & role)
            def _():
                stage(u)

        run(stage_mid, LAG_MID, is_mid)
        run(stage_near, LAG_NEAR, is_mid)
        run(stage_relay, LAG_RELAY, is_mid)
        run(stage_one, LAG_ONE)
        @pl.when(s == LAG_ONE)
        def _():
            @pl.when(is_mid)
            def _():
                give().wait_recv()
                give_on().wait_recv()
                for k in range(1, cols):
                    spread(k, my_col).start()

            for k in range(1, cols):
                t_rows(2, last, k, my_col, own_side).start()

        run(stage_zero, 0)
        for m in range(nodes_here):

            @pl.when(is_end & (s == LAG_FAR + m * chunks))
            def _(m=m):
                stage_far(m)

        run(stage_end, LAG_END, is_end)
        return 0

    lax.fori_loop(0, units + max(LAG_NEAR, LAG_END), step, 0)

    sent(TO_TWO, held.at[:, 0], held.at[:, 1])
    sent(FORWARD, held, theirs)

    @pl.when(is_mid)
    def _():
        early = pl.ds(0, plain)
        late = pl.ds(plain, units - plain)
        sent(TO_ACROSS, y1.at[early], across.at[early])
        sent(RELAY, pair.at[early], relayed.at[early])
        sent(PARTIAL, partial_out, partial_in)
        sent(SUM_NEAR, sums.at[0], across.at[late])
        sent(SUM_FAR, sums.at[1], across.at[late])
        give().wait_send()
        give_on().wait_send()
        for k in range(1, cols):
            spread(k, my_col).wait_send()

    @pl.when(is_end)
    def _():
        sent(TO_PAIR, y1, pair)
        whole = t_far.at[pl.ds(0, last)]
        remote(whole, whole, far_send.at[0], far_recv.at[0], {"node": by_pair}).wait_send()
        far(last).wait_send()
        give_pair().wait_send()

    for k in range(1, cols):
        beside = {"col": (my_col + k) % cols}
        both, rest = t_in.at[pl.ds(0, 2)], t_in.at[2, pl.ds(0, last)]
        remote(both, t.at[pl.ds(0, 2), :, :, my_rows, :], t_send.at[0, k - 1], t_recv.at[0, 0, k - 1], beside).wait_send()
        remote(
            rest, t.at[2, pl.ds(0, last), :, my_rows, :], t_send.at[1, k - 1], t_recv.at[0, 0, k - 1], beside
        ).wait_send()
        t_rows(2, last, k, my_col, own_side).wait_send()


def local(coefficients, transfer):
    cols = lax.axis_size("col")
    nodes_here, rank, columns = coefficients.shape
    levels, _, children, rows, _ = transfer.shape
    width = min(WIDTH, columns)
    chunks = columns // width
    units = nodes_here * chunks
    plain = units - chunks
    others = max(cols - 1, 1)
    kind = coefficients.dtype
    block = (rank, width)
    dma = pltpu.SemaphoreType.DMA
    return pl.pallas_call(
        functools.partial(kernel, cols, chunks),
        out_shape=pltpu.VMEM(coefficients.shape, kind),
        in_specs=[pl.BlockSpec(memory_space=pl.ANY)] * 2,
        out_specs=pl.BlockSpec(memory_space=pltpu.VMEM),
        scratch_shapes=[
            pltpu.VMEM(coefficients.shape, kind),
            pltpu.VMEM((levels, nodes_here, children, rank, rank), kind),
            pltpu.VMEM((nodes_here, children - 1, rank, rank), kind),
            pltpu.VMEM((2, rows, rank), kind),
            pltpu.VMEM((2, 2, rank, rank), kind),
            pltpu.VMEM((units, 2) + block, kind),
            pltpu.VMEM((units, 2) + block, kind),
            pltpu.VMEM((units,) + block, kind),
            pltpu.VMEM((units,) + block, kind),
            pltpu.VMEM((units,) + block, kind),
            pltpu.VMEM((units,) + block, kind),
            pltpu.VMEM((units,) + block, kind),
            pltpu.VMEM((units,) + block, kind),
            pltpu.VMEM((2, chunks) + block, kind),
            dma((2,)),
            dma((8,)),
            dma((5, units)),
            dma((3, others)),
            dma((levels, nodes_here, others)),
            dma((2,)),
            dma((nodes_here,)),
            dma((2,)),
            dma((3,)),
            dma((others,)),
            dma((others,)),
        ],
        compiler_params=pltpu.CompilerParams(
            collective_id=0, has_side_effects=True, vmem_limit_bytes=56 * 1024 * 1024
        ),
    )(coefficients, transfer)


def solution(mesh):
    return jax.shard_map(
        local,
        mesh=mesh,
        in_specs=(P("node", None, "col"), P(None, "node", None, "col", None)),
        out_specs=P("node", None, "col"),
        check_vma=False,
    )
```

```python
import functools

import jax
import jax.numpy as jnp
from jax import lax
from jax.experimental import pallas as pl
from jax.experimental.pallas import tpu as pltpu
from jax.sharding import PartitionSpec as P

MESH = pl.DeviceIdType.MESH
WIDTH = 256
HELD_BACK = 4
LAG_ONE, LAG_RELAY, LAG_FAR, LAG_MID, LAG_NEAR, LAG_END = 2, 4, 5, 8, 12, 10
TO_TWO, FORWARD, TO_PAIR, TO_ACROSS, RELAY, PARTIAL, SUM_NEAR, SUM_FAR = range(8)
ROW = {TO_TWO: 0, FORWARD: 1, TO_PAIR: 2, TO_ACROSS: 3, RELAY: 4, PARTIAL: 3, SUM_NEAR: 3, SUM_FAR: 4}


def flip(i, bit):
    return i + bit - 2 * bit * (i // bit % 2)


def dot(a, b):
    return jnp.dot(a, b, preferred_element_type=jnp.float32)


def kernel(
    cols, chunks, x_in, t_in, out_ref,
    x, t, t_far, t_pass, t_sum, held, theirs, y1, pair, across, relayed, partial_out, partial_in, sums,
    local_sem, send, recv, half_x, half_core, t_send, t_recv, far_send, far_recv, sum_send, sum_recv, spread_send, spread_recv,
):
    nodes_here = x_in.shape[0]
    last = nodes_here - 1
    rows = t_in.shape[3]
    units = nodes_here * chunks
    plain = last * chunks
    width = x_in.shape[2] // chunks
    me = lax.axis_index("node")
    my_col = lax.axis_index("col")
    one = me % 4
    two = me // 4 % 4
    side = two // 2 * 2
    other = 2 - side
    is_mid = (two + 1) // 2 % 2 == 1
    is_end = (two + 1) // 2 % 2 == 0
    by_core, by_two, by_pair = flip(me, 1), flip(me, 2), flip(me, 4)
    by_across = flip(by_pair, 8)
    my_rows = pl.ds(my_col * rows, rows)

    x_copy = pltpu.make_async_copy(x_in, x, local_sem.at[0])
    x_copy.start()
    t_copy = pltpu.make_async_copy(t_in, t.at[:, :, :, my_rows, :], local_sem.at[1])
    t_copy.start()

    barrier = pltpu.get_barrier_semaphore()
    for k in range(1, cols):
        pl.semaphore_signal(barrier, inc=1, device_id={"col": (my_col + k) % cols}, device_id_type=MESH)
    for device in (by_pair, by_two, by_core):
        pl.semaphore_signal(barrier, inc=1, device_id={"node": device}, device_id_type=MESH)

    @pl.when(is_mid)
    def _():
        pl.semaphore_signal(barrier, inc=1, device_id={"node": by_across}, device_id_type=MESH)
        pl.semaphore_wait(barrier, 4 + cols - 1)

    @pl.when(is_end)
    def _():
        pl.semaphore_wait(barrier, 3 + cols - 1)

    def remote(source, target, send_sem, recv_sem, device):
        return pltpu.make_async_remote_copy(
            src_ref=source, dst_ref=target, send_sem=send_sem, recv_sem=recv_sem,
            device_id=device, device_id_type=MESH,
        )

    def t_rows(level, m, k, col, children=None):
        here = pl.ds(col * rows, rows)
        if children is None:
            source, target = t_in.at[level, m], t.at[level, m, :, here, :]
        else:
            source, target = t_in.at[level, m, children], t.at[level, m, children, here, :]
        group = 0 if level < 2 else 1 if children is None else 2
        return remote(
            source, target, t_send.at[group, k - 1], t_recv.at[level, m, k - 1], {"col": (my_col + k) % cols}
        )

    def wait_rows(level, m, children=None):
        for k in range(1, cols):
            t_rows(level, m, k, (my_col + cols - k) % cols, children).wait_recv()

    own_side = pl.ds(side, 2)

    order = sorted(
        (3 * m + 2 * level, level, m) for m in range(nodes_here) for level in range(3) if (level, m) != (2, last)
    )
    for _, level, m in order:
        for k in range(1, cols):
            t_rows(level, m, k, my_col).start()

    given = t_in.at[2, last, pl.ds(other, 2)]

    def give():
        return remote(given, t_sum.at[0, :, my_rows, :], sum_send.at[0], sum_recv.at[0], {"node": by_across})

    def give_pair():
        return remote(given, t_pass, sum_send.at[0], sum_recv.at[2], {"node": by_pair})

    def give_on():
        return remote(t_pass, t_sum.at[1, :, my_rows, :], sum_send.at[1], sum_recv.at[1], {"node": by_across})

    @pl.when(is_mid)
    def _():
        give().start()

    @pl.when(is_end)
    def _():
        give_pair().start()

    def spread(k, col):
        part = t_sum.at[:, :, pl.ds(col * rows, rows), :]
        return remote(part, part, spread_send.at[k - 1], spread_recv.at[k - 1], {"col": (my_col + k) % cols})

    def copy(kind, u):
        source, target, device = {
            TO_TWO: lambda: (held.at[u, 0], held.at[u, 1], by_two),
            FORWARD: lambda: (held.at[u], theirs.at[u], by_core),
            TO_PAIR: lambda: (y1.at[u], pair.at[u], by_pair),
            TO_ACROSS: lambda: (y1.at[u], across.at[u], by_across),
            RELAY: lambda: (pair.at[u], relayed.at[u], by_across),
            PARTIAL: lambda: (partial_out.at[u], partial_in.at[u], by_pair),
            SUM_NEAR: lambda: (sums.at[0, u - plain], across.at[u], by_across),
            SUM_FAR: lambda: (sums.at[1, u - plain], relayed.at[u], by_across),
        }[kind]()
        return remote(source, target, send.at[kind], recv.at[ROW[kind], u], {"node": device})

    def sent(kind, source, target):
        remote(source, target, send.at[kind], recv.at[ROW[kind], 0], {"node": by_pair}).wait_send()

    def far(m):
        if isinstance(m, int) and m == last:
            source, target, sem = t.at[2, m, flip(two, 1)], t_far.at[m, 0], far_send.at[1]
        else:
            source, target, sem = t.at[2, m, pl.ds(1 - two // 3, 3)], t_far.at[m], far_send.at[0]
        return remote(source, target, sem, far_recv.at[m], {"node": by_pair})

    def store(u, total):
        columns = pl.ds(pl.multiple_of(u % chunks * width, width), width)
        out_ref[u // chunks, :, columns] = total.astype(out_ref.dtype)

    def first(u, action):
        @pl.when(u % chunks == 0)
        def _():
            action(u // chunks)

    def all_columns(u):
        return pl.ds(pl.multiple_of(u % chunks * width, width), width)

    def piece_to_two(u, here, columns, sem):
        return remote(held.at[u, 0, here, columns], held.at[u, 1, here, columns], send.at[TO_TWO], sem, {"node": by_two})

    def zero_rows(u, here, wanted, columns, sem):
        total = dot(t[0, 0, 0, here], x[0, :, wanted])
        for j in range(1, 4):
            total += dot(t[0, 0, j, here], x[j, :, wanted])
        held[u, 0, here, columns] = total.astype(held.dtype)
        piece_to_two(u, here, columns, sem).start()

    def rows_of(k):
        return pl.ds(pl.multiple_of((my_col + k) % cols * rows, rows), rows)

    whole = pl.ds(0, width)

    def own_rows(u, _):
        zero_rows(u, rows_of(0), all_columns(u), whole, recv.at[ROW[TO_TWO], u])
        return 0

    def other_rows(u, _):
        for k in range(1, cols):
            zero_rows(u, rows_of(k), all_columns(u), whole, recv.at[ROW[TO_TWO], u])
        return 0

    halves = [pl.ds(h * width // 2, width // 2) for h in range(2)]

    def half_to_core(h):
        source, target = held.at[0, :, :, halves[h]], theirs.at[0, :, :, halves[h]]
        return remote(source, target, send.at[FORWARD], half_core.at[h], {"node": by_core})

    def one_rows(here, columns):
        total = dot(t[1, 0, one, here], held[0, 0, :, columns])
        total += dot(t[1, 0, flip(one, 2), here], held[0, 1, :, columns])
        total += dot(t[1, 0, flip(one, 1), here], theirs[0, 0, :, columns])
        total += dot(t[1, 0, 3 - one, here], theirs[0, 1, :, columns])
        y1[0, here, columns] = total.astype(y1.dtype)

        def part(kind, target, device):
            remote(
                y1.at[0, here, columns], target.at[0, here, columns],
                send.at[kind], recv.at[ROW[kind], 0], {"node": device},
            ).start()

        pl.when(is_mid)(lambda: part(TO_ACROSS, across, by_across))
        pl.when(is_end)(lambda: part(TO_PAIR, pair, by_pair))

    def first_unit():
        wait_rows(0, 0)
        for h in range(2):
            for k in range(1, cols):
                zero_rows(0, rows_of(k), halves[h], halves[h], half_x.at[h, k - 1])
        lax.fori_loop(1, chunks, other_rows, 0)
        piece_to_two(0, rows_of(0), whole, recv.at[ROW[TO_TWO], 0]).wait_recv()
        for h in range(2):
            for k in range(1, cols):
                piece_to_two(0, rows_of(k), halves[h], half_x.at[h, k - 1]).wait_recv()
            half_to_core(h).start()
        for h in range(2):
            half_to_core(h).wait_recv()
            one_rows(rows_of(0), halves[h])
        wait_rows(1, 0)
        for k in range(1, cols):
            one_rows(rows_of(k), whole)

    def stage_zero(u):
        first(u, lambda m: wait_rows(0, m))
        m = u // chunks
        columns = all_columns(u)
        total = dot(t[0, m, 0], x[0, :, columns])
        for j in range(1, 4):
            total += dot(t[0, m, j], x[j, :, columns])
        held[u, 0] = total.astype(held.dtype)
        copy(TO_TWO, u).start()

    def stage_one(u):
        copy(TO_TWO, u).wait_recv()
        copy(FORWARD, u).start()
        first(u, lambda m: wait_rows(1, m))
        m = u // chunks
        total = dot(t[1, m, one], held[u, 0])
        total += dot(t[1, m, flip(one, 2)], held[u, 1])
        copy(FORWARD, u).wait_recv()
        total += dot(t[1, m, flip(one, 1)], theirs[u, 0])
        total += dot(t[1, m, 3 - one], theirs[u, 1])
        y1[u] = total.astype(y1.dtype)

        @pl.when(is_mid & (u < plain))
        def _():
            copy(TO_ACROSS, u).start()

        @pl.when(is_end)
        def _():
            copy(TO_PAIR, u).start()

    def stage_relay(u):
        copy(TO_PAIR, u).wait_recv()

        @pl.when(u < plain)
        def _():
            copy(RELAY, u).start()

        @pl.when(u >= plain)
        def _():
            @pl.when(u == plain)
            def _():
                for k in range(1, cols):
                    spread(k, (my_col + cols - k) % cols).wait_recv()

            for who, kind in ((1, SUM_FAR), (0, SUM_NEAR)):
                total = dot(t_sum[who, two % 2], y1[u]) + dot(t_sum[who, 1 - two % 2], pair[u])
                sums[who, u - plain] = total.astype(sums.dtype)
                if kind == SUM_FAR:
                    copy(kind, u).start()

            @pl.when(u < units - HELD_BACK)
            def _():
                copy(SUM_NEAR, u).start()

            @pl.when(u == units - 1)
            def _():
                for late in range(min(HELD_BACK, chunks), 0, -1):
                    copy(SUM_NEAR, units - late).start()

    def stage_far(m):
        wait_rows(2, m, own_side if m == last else None)
        far(m).start()

    def own_part(u):
        m = u // chunks
        return dot(t[2, m, two], y1[u])

    def pair_part(u):
        return dot(t[2, u // chunks, flip(two, 1)], pair[u])

    def stage_mid(u):
        @pl.when(u < plain)
        def _():
            def arrive(m):
                wait_rows(2, m)
                far(m).wait_recv()

            first(u, arrive)
            m = u // chunks
            copy(TO_ACROSS, u).wait_recv()
            copy(RELAY, u).wait_recv()
            start = 1 - two // 2
            part = dot(t_far[m, 3 - two - start], across[u])
            part += dot(t_far[m, flip(3 - two, 1) - start], relayed[u])
            part += dot(t_far[m, two - start], y1[u])
            partial_out[u] = part.astype(partial_out.dtype)
            copy(PARTIAL, u).start()
            total = own_part(u) + pair_part(u)
            total += dot(t[2, m, 3 - two], across[u])
            total += dot(t[2, m, flip(two, 2)], relayed[u])
            store(u, total)

        @pl.when(u >= plain)
        def _():
            @pl.when(u == plain)
            def _():
                wait_rows(2, last, own_side)
                far(last).wait_recv()

            copy(SUM_FAR, u).wait_recv()
            part = dot(t_far[last, 0], y1[u]) + relayed[u].astype(jnp.float32)
            partial_out[u] = part.astype(partial_out.dtype)
            copy(PARTIAL, u).start()

    def stage_near(u):
        @pl.when(u >= plain)
        def _():
            total = own_part(u) + pair_part(u)
            copy(SUM_NEAR, u).wait_recv()
            store(u, total + across[u].astype(jnp.float32))

    def stage_end(u):
        total = own_part(u)
        copy(PARTIAL, u).wait_recv()
        store(u, total + partial_in[u].astype(jnp.float32))

    x_copy.wait()
    t_copy.wait()
    lax.fori_loop(0, chunks, own_rows, 0)

    @pl.when(is_mid)
    def _():
        give_pair().wait_recv()
        give_on().start()

    first_unit()

    def step(s, _):
        def run(stage, lag, role=None, start=0):
            u = s - lag
            ready = (u >= start) & (u < units)

            @pl.when(ready if role is None else ready & role)
            def _():
                stage(u)

        run(stage_mid, LAG_MID, is_mid)
        run(stage_near, LAG_NEAR, is_mid)
        run(stage_relay, LAG_RELAY, is_mid)
        run(stage_one, LAG_ONE, start=1)
        @pl.when(s == LAG_ONE + 1)
        def _():
            @pl.when(is_mid)
            def _():
                give().wait_recv()
                give_on().wait_recv()
                for k in range(1, cols):
                    spread(k, my_col).start()

            for k in range(1, cols):
                t_rows(2, last, k, my_col, own_side).start()

        run(stage_zero, 0, start=chunks)
        for m in range(nodes_here):

            @pl.when(is_end & (s == LAG_FAR + m * chunks))
            def _(m=m):
                stage_far(m)

        run(stage_end, LAG_END, is_end)
        return 0

    lax.fori_loop(LAG_ONE + 1, units + max(LAG_NEAR, LAG_END), step, 0)

    sent(TO_TWO, held.at[:, 0], held.at[:, 1])
    sent(FORWARD, held, theirs)

    @pl.when(is_mid)
    def _():
        early = pl.ds(0, plain)
        late = pl.ds(plain, units - plain)
        sent(TO_ACROSS, y1.at[early], across.at[early])
        sent(RELAY, pair.at[early], relayed.at[early])
        sent(PARTIAL, partial_out, partial_in)
        sent(SUM_NEAR, sums.at[0], across.at[late])
        sent(SUM_FAR, sums.at[1], across.at[late])
        give().wait_send()
        give_on().wait_send()
        for k in range(1, cols):
            spread(k, my_col).wait_send()

    @pl.when(is_end)
    def _():
        sent(TO_PAIR, y1, pair)
        full = t_far.at[pl.ds(0, last)]
        remote(full, full, far_send.at[0], far_recv.at[0], {"node": by_pair}).wait_send()
        far(last).wait_send()
        give_pair().wait_send()

    for k in range(1, cols):
        beside = {"col": (my_col + k) % cols}
        both, rest = t_in.at[pl.ds(0, 2)], t_in.at[2, pl.ds(0, last)]
        remote(both, t.at[pl.ds(0, 2), :, :, my_rows, :], t_send.at[0, k - 1], t_recv.at[0, 0, k - 1], beside).wait_send()
        remote(
            rest, t.at[2, pl.ds(0, last), :, my_rows, :], t_send.at[1, k - 1], t_recv.at[0, 0, k - 1], beside
        ).wait_send()
        t_rows(2, last, k, my_col, own_side).wait_send()


def local(coefficients, transfer):
    cols = lax.axis_size("col")
    nodes_here, rank, columns = coefficients.shape
    levels, _, children, rows, _ = transfer.shape
    width = min(WIDTH, columns)
    chunks = columns // width
    units = nodes_here * chunks
    plain = units - chunks
    others = max(cols - 1, 1)
    kind = coefficients.dtype
    block = (rank, width)
    dma = pltpu.SemaphoreType.DMA
    return pl.pallas_call(
        functools.partial(kernel, cols, chunks),
        out_shape=pltpu.VMEM(coefficients.shape, kind),
        in_specs=[pl.BlockSpec(memory_space=pl.ANY)] * 2,
        out_specs=pl.BlockSpec(memory_space=pltpu.VMEM),
        scratch_shapes=[
            pltpu.VMEM(coefficients.shape, kind),
            pltpu.VMEM((levels, nodes_here, children, rank, rank), kind),
            pltpu.VMEM((nodes_here, children - 1, rank, rank), kind),
            pltpu.VMEM((2, rows, rank), kind),
            pltpu.VMEM((2, 2, rank, rank), kind),
            pltpu.VMEM((units, 2) + block, kind),
            pltpu.VMEM((units, 2) + block, kind),
            pltpu.VMEM((units,) + block, kind),
            pltpu.VMEM((units,) + block, kind),
            pltpu.VMEM((units,) + block, kind),
            pltpu.VMEM((units,) + block, kind),
            pltpu.VMEM((units,) + block, kind),
            pltpu.VMEM((units,) + block, kind),
            pltpu.VMEM((2, chunks) + block, kind),
            dma((2,)),
            dma((8,)),
            dma((5, units)),
            dma((2, others)),
            dma((2,)),
            dma((3, others)),
            dma((levels, nodes_here, others)),
            dma((2,)),
            dma((nodes_here,)),
            dma((2,)),
            dma((3,)),
            dma((others,)),
            dma((others,)),
        ],
        compiler_params=pltpu.CompilerParams(
            collective_id=0, has_side_effects=True, vmem_limit_bytes=56 * 1024 * 1024
        ),
    )(coefficients, transfer)


def solution(mesh):
    return jax.shard_map(
        local,
        mesh=mesh,
        in_specs=(P("node", None, "col"), P(None, "node", None, "col", None)),
        out_specs=P("node", None, "col"),
        check_vma=False,
    )
```

```python
import functools

import jax
import jax.numpy as jnp
from jax import lax
from jax.experimental import pallas as pl
from jax.experimental.pallas import tpu as pltpu
from jax.sharding import PartitionSpec as P

MESH = pl.DeviceIdType.MESH
WIDTH = 256
HELD_BACK = 4
LAG_ONE, LAG_RELAY, LAG_FAR, LAG_MID, LAG_NEAR, LAG_END = 2, 4, 5, 8, 12, 12
TO_TWO, FORWARD, TO_PAIR, TO_ACROSS, RELAY, PARTIAL, SUM_NEAR, SUM_FAR = range(8)
ROW = {TO_TWO: 0, FORWARD: 1, TO_PAIR: 2, TO_ACROSS: 3, RELAY: 3, PARTIAL: 3, SUM_NEAR: 3, SUM_FAR: 3}


def flip(i, bit):
    return i + bit - 2 * bit * (i // bit % 2)


def dot(a, b):
    return jnp.dot(a, b, preferred_element_type=jnp.float32)


def kernel(
    cols, chunks, x_in, t_in, out_ref,
    x, t, t_far, t_pass, t_sum, held, theirs, y1, pair, come, partial_out, partial_in, sums,
    local_sem, send, recv, far_sum, half_x, half_core, t_send, t_recv, far_send, far_recv, sum_send, sum_recv, spread_send, spread_recv,
):
    nodes_here = x_in.shape[0]
    last = nodes_here - 1
    rows = t_in.shape[3]
    units = nodes_here * chunks
    plain = last * chunks
    width = x_in.shape[2] // chunks
    me = lax.axis_index("node")
    my_col = lax.axis_index("col")
    one = me % 4
    two = me // 4 % 4
    side = two // 2 * 2
    other = 2 - side
    is_mid = (two + 1) // 2 % 2 == 1
    is_end = (two + 1) // 2 % 2 == 0
    by_core, by_two, by_pair = flip(me, 1), flip(me, 2), flip(me, 4)
    by_across = flip(by_pair, 8)
    my_rows = pl.ds(my_col * rows, rows)

    barrier = pltpu.get_barrier_semaphore()
    for k in range(1, cols):
        pl.semaphore_signal(barrier, inc=1, device_id={"col": (my_col + k) % cols}, device_id_type=MESH)
    for device in (by_pair, by_two, by_core):
        pl.semaphore_signal(barrier, inc=1, device_id={"node": device}, device_id_type=MESH)

    @pl.when(is_mid)
    def _():
        pl.semaphore_signal(barrier, inc=1, device_id={"node": by_across}, device_id_type=MESH)

    x_copy = pltpu.make_async_copy(x_in, x, local_sem.at[0])
    x_copy.start()
    t_copy = pltpu.make_async_copy(t_in, t.at[:, :, :, my_rows, :], local_sem.at[1])
    t_copy.start()

    @pl.when(is_mid)
    def _():
        pl.semaphore_wait(barrier, 4 + cols - 1)

    @pl.when(is_end)
    def _():
        pl.semaphore_wait(barrier, 3 + cols - 1)

    def remote(source, target, send_sem, recv_sem, device):
        return pltpu.make_async_remote_copy(
            src_ref=source, dst_ref=target, send_sem=send_sem, recv_sem=recv_sem,
            device_id=device, device_id_type=MESH,
        )

    def t_rows(level, m, k, col, children=None):
        here = pl.ds(col * rows, rows)
        if children is None:
            source, target = t_in.at[level, m], t.at[level, m, :, here, :]
        else:
            source, target = t_in.at[level, m, children], t.at[level, m, children, here, :]
        group = 0 if level < 2 else 1 if children is None else 2
        return remote(
            source, target, t_send.at[group, k - 1], t_recv.at[level, m, k - 1], {"col": (my_col + k) % cols}
        )

    def wait_rows(level, m, children=None):
        for k in range(1, cols):
            t_rows(level, m, k, (my_col + cols - k) % cols, children).wait_recv()

    own_side = pl.ds(side, 2)

    order = sorted(
        (3 * m + 2 * level, level, m) for m in range(nodes_here) for level in range(3) if (level, m) != (2, last)
    )
    for _, level, m in order:
        for k in range(1, cols):
            t_rows(level, m, k, my_col).start()

    given = t_in.at[2, last, pl.ds(other, 2)]

    def give():
        return remote(given, t_sum.at[0, :, my_rows, :], sum_send.at[0], sum_recv.at[0], {"node": by_across})

    def give_pair():
        return remote(given, t_pass, sum_send.at[0], sum_recv.at[2], {"node": by_pair})

    def give_on():
        return remote(t_pass, t_sum.at[1, :, my_rows, :], sum_send.at[1], sum_recv.at[1], {"node": by_across})

    @pl.when(is_mid)
    def _():
        give().start()

    @pl.when(is_end)
    def _():
        give_pair().start()

    def spread(k, col):
        part = t_sum.at[:, :, pl.ds(col * rows, rows), :]
        return remote(part, part, spread_send.at[k - 1], spread_recv.at[k - 1], {"col": (my_col + k) % cols})

    def copy(kind, u):
        source, target, device = {
            TO_TWO: lambda: (held.at[u, 0], held.at[u, 1], by_two),
            FORWARD: lambda: (held.at[u], theirs.at[u], by_core),
            TO_PAIR: lambda: (y1.at[u], pair.at[u], by_pair),
            TO_ACROSS: lambda: (y1.at[u], come.at[u, 0], by_across),
            RELAY: lambda: (pair.at[u], come.at[u, 1], by_across),
            PARTIAL: lambda: (partial_out.at[u], partial_in.at[u], by_pair),
            SUM_NEAR: lambda: (sums.at[0, u - plain], come.at[u, 0], by_across),
            SUM_FAR: lambda: (sums.at[1, u - plain], come.at[u, 1], by_across),
        }[kind]()
        sem = far_sum.at[u - plain] if kind == SUM_FAR else recv.at[ROW[kind], u]
        return remote(source, target, send.at[kind], sem, {"node": device})

    def sent(kind, source, target):
        remote(source, target, send.at[kind], recv.at[ROW[kind], 0], {"node": by_pair}).wait_send()

    def far(m):
        if isinstance(m, int) and m == last:
            source, target, sem = t.at[2, m, flip(two, 1)], t_far.at[m, 0], far_send.at[1]
        else:
            source, target, sem = t.at[2, m, pl.ds(1 - two // 3, 3)], t_far.at[m], far_send.at[0]
        return remote(source, target, sem, far_recv.at[m], {"node": by_pair})

    def store(u, total):
        columns = pl.ds(pl.multiple_of(u % chunks * width, width), width)
        out_ref[u // chunks, :, columns] = total.astype(out_ref.dtype)

    def first(u, action):
        @pl.when(u % chunks == 0)
        def _():
            action(u // chunks)

    def all_columns(u):
        return pl.ds(pl.multiple_of(u % chunks * width, width), width)

    def piece_to_two(u, here, columns, sem):
        return remote(held.at[u, 0, here, columns], held.at[u, 1, here, columns], send.at[TO_TWO], sem, {"node": by_two})

    def zero_rows(u, here, wanted, columns, sem):
        total = dot(t[0, 0, 0, here], x[0, :, wanted])
        for j in range(1, 4):
            total += dot(t[0, 0, j, here], x[j, :, wanted])
        held[u, 0, here, columns] = total.astype(held.dtype)
        piece_to_two(u, here, columns, sem).start()

    def rows_of(k):
        return pl.ds(pl.multiple_of((my_col + k) % cols * rows, rows), rows)

    whole = pl.ds(0, width)

    def own_rows(u, _):
        zero_rows(u, rows_of(0), all_columns(u), whole, recv.at[ROW[TO_TWO], u])
        return 0

    def other_rows(u, _):
        for k in range(1, cols):
            zero_rows(u, rows_of(k), all_columns(u), whole, recv.at[ROW[TO_TWO], u])
        return 0

    halves = [pl.ds(h * width // 2, width // 2) for h in range(2)]

    def half_to_core(h):
        source, target = held.at[0, :, :, halves[h]], theirs.at[0, :, :, halves[h]]
        return remote(source, target, send.at[FORWARD], half_core.at[h], {"node": by_core})

    def one_rows(here, columns):
        total = dot(t[1, 0, one, here], held[0, 0, :, columns])
        total += dot(t[1, 0, flip(one, 2), here], held[0, 1, :, columns])
        total += dot(t[1, 0, flip(one, 1), here], theirs[0, 0, :, columns])
        total += dot(t[1, 0, 3 - one, here], theirs[0, 1, :, columns])
        y1[0, here, columns] = total.astype(y1.dtype)

        def part(kind, target, device):
            remote(
                y1.at[0, here, columns], target.at[here, columns],
                send.at[kind], recv.at[ROW[kind], 0], {"node": device},
            ).start()

        pl.when(is_mid)(lambda: part(TO_ACROSS, come.at[0, 0], by_across))
        pl.when(is_end)(lambda: part(TO_PAIR, pair.at[0], by_pair))

    def forward(u):
        copy(TO_TWO, u).wait_recv()
        copy(FORWARD, u).start()

    def first_unit():
        wait_rows(0, 0)
        for h in range(2):
            for k in range(1, cols):
                zero_rows(0, rows_of(k), halves[h], halves[h], half_x.at[h, k - 1])
        lax.fori_loop(1, chunks, other_rows, 0)
        piece_to_two(0, rows_of(0), whole, recv.at[ROW[TO_TWO], 0]).wait_recv()
        for h in range(2):
            for k in range(1, cols):
                piece_to_two(0, rows_of(k), halves[h], half_x.at[h, k - 1]).wait_recv()
            half_to_core(h).start()
        for h in range(2):
            half_to_core(h).wait_recv()
            one_rows(rows_of(0), halves[h])
        if chunks > 1:
            forward(1)
        wait_rows(1, 0)
        for k in range(1, cols):
            one_rows(rows_of(k), whole)

    def stage_zero(u):
        first(u, lambda m: wait_rows(0, m))
        m = u // chunks
        columns = all_columns(u)
        total = dot(t[0, m, 0], x[0, :, columns])
        for j in range(1, 4):
            total += dot(t[0, m, j], x[j, :, columns])
        held[u, 0] = total.astype(held.dtype)
        copy(TO_TWO, u).start()

    def stage_one(u):
        pl.when(u > (1 if chunks > 1 else 0))(lambda: forward(u))
        first(u, lambda m: wait_rows(1, m))
        m = u // chunks
        total = dot(t[1, m, one], held[u, 0])
        total += dot(t[1, m, flip(one, 2)], held[u, 1])
        copy(FORWARD, u).wait_recv()
        total += dot(t[1, m, flip(one, 1)], theirs[u, 0])
        total += dot(t[1, m, 3 - one], theirs[u, 1])
        y1[u] = total.astype(y1.dtype)

        @pl.when(is_mid & (u < plain))
        def _():
            copy(TO_ACROSS, u).start()

        @pl.when(is_end)
        def _():
            copy(TO_PAIR, u).start()

    def stage_relay(u):
        copy(TO_PAIR, u).wait_recv()

        @pl.when(u < plain)
        def _():
            copy(RELAY, u).start()

        @pl.when(u >= plain)
        def _():
            @pl.when(u == plain)
            def _():
                for k in range(1, cols):
                    spread(k, (my_col + cols - k) % cols).wait_recv()

            for who, kind in ((1, SUM_FAR), (0, SUM_NEAR)):
                total = dot(t_sum[who, two % 2], y1[u]) + dot(t_sum[who, 1 - two % 2], pair[u])
                sums[who, u - plain] = total.astype(sums.dtype)
                if kind == SUM_FAR:
                    copy(kind, u).start()

            @pl.when(u < units - HELD_BACK)
            def _():
                copy(SUM_NEAR, u).start()

            @pl.when(u == units - 1)
            def _():
                for late in range(min(HELD_BACK, chunks), 0, -1):
                    copy(SUM_NEAR, units - late).start()

    def stage_far(m):
        wait_rows(2, m, own_side if m == last else None)
        far(m).start()

    def own_part(u):
        m = u // chunks
        return dot(t[2, m, two], y1[u])

    def pair_part(u):
        return dot(t[2, u // chunks, flip(two, 1)], pair[u])

    def stage_mid(u):
        @pl.when(u < plain)
        def _():
            def arrive(m):
                wait_rows(2, m)
                far(m).wait_recv()

            first(u, arrive)
            m = u // chunks
            remote(come.at[u], come.at[u], send.at[RELAY], recv.at[ROW[RELAY], u], {"node": by_across}).wait_recv()
            start = 1 - two // 2
            part = dot(t_far[m, 3 - two - start], come[u, 0])
            part += dot(t_far[m, flip(3 - two, 1) - start], come[u, 1])
            part += dot(t_far[m, two - start], y1[u])
            partial_out[u] = part.astype(partial_out.dtype)
            copy(PARTIAL, u).start()
            total = own_part(u) + pair_part(u)
            total += dot(t[2, m, 3 - two], come[u, 0])
            total += dot(t[2, m, flip(two, 2)], come[u, 1])
            store(u, total)

        @pl.when(u >= plain)
        def _():
            @pl.when(u == plain)
            def _():
                wait_rows(2, last, own_side)
                far(last).wait_recv()

            copy(SUM_FAR, u).wait_recv()
            part = dot(t_far[last, 0], y1[u]) + come[u, 1].astype(jnp.float32)
            partial_out[u] = part.astype(partial_out.dtype)
            copy(PARTIAL, u).start()

    def stage_near(u):
        @pl.when(u >= plain)
        def _():
            total = own_part(u) + pair_part(u)
            copy(SUM_NEAR, u).wait_recv()
            store(u, total + come[u, 0].astype(jnp.float32))

    def stage_end(u):
        total = own_part(u)
        copy(PARTIAL, u).wait_recv()
        store(u, total + partial_in[u].astype(jnp.float32))

    x_copy.wait()
    t_copy.wait()
    lax.fori_loop(0, chunks, own_rows, 0)

    @pl.when(is_mid)
    def _():
        give_pair().wait_recv()
        give_on().start()

    first_unit()

    def step(s, _):
        def run(stage, lag, role=None, start=0):
            u = s - lag
            ready = (u >= start) & (u < units)

            @pl.when(ready if role is None else ready & role)
            def _():
                stage(u)

        run(stage_mid, LAG_MID, is_mid)
        run(stage_near, LAG_NEAR, is_mid)
        run(stage_relay, LAG_RELAY, is_mid)
        run(stage_one, LAG_ONE, start=1)
        @pl.when(s == LAG_ONE + 1)
        def _():
            @pl.when(is_mid)
            def _():
                give().wait_recv()
                give_on().wait_recv()
                for k in range(1, cols):
                    spread(k, my_col).start()

            for k in range(1, cols):
                t_rows(2, last, k, my_col, own_side).start()

        run(stage_zero, 0, start=chunks)
        for m in range(nodes_here):

            @pl.when(is_end & (s == LAG_FAR + m * chunks))
            def _(m=m):
                stage_far(m)

        run(stage_end, LAG_END, is_end)
        return 0

    lax.fori_loop(LAG_ONE + 1, units + max(LAG_NEAR, LAG_END), step, 0)

    sent(TO_TWO, held.at[:, 0], held.at[:, 1])
    sent(FORWARD, held, theirs)

    @pl.when(is_mid)
    def _():
        early = pl.ds(0, plain)
        late = pl.ds(plain, units - plain)
        sent(TO_ACROSS, y1.at[early], come.at[early, 0])
        sent(RELAY, pair.at[early], come.at[early, 1])
        sent(PARTIAL, partial_out, partial_in)
        sent(SUM_NEAR, sums.at[0], come.at[late, 0])
        sent(SUM_FAR, sums.at[1], come.at[late, 0])
        give().wait_send()
        give_on().wait_send()
        for k in range(1, cols):
            spread(k, my_col).wait_send()

    @pl.when(is_end)
    def _():
        sent(TO_PAIR, y1, pair)
        full = t_far.at[pl.ds(0, last)]
        remote(full, full, far_send.at[0], far_recv.at[0], {"node": by_pair}).wait_send()
        far(last).wait_send()
        give_pair().wait_send()

    for k in range(1, cols):
        beside = {"col": (my_col + k) % cols}
        both, rest = t_in.at[pl.ds(0, 2)], t_in.at[2, pl.ds(0, last)]
        remote(both, t.at[pl.ds(0, 2), :, :, my_rows, :], t_send.at[0, k - 1], t_recv.at[0, 0, k - 1], beside).wait_send()
        remote(
            rest, t.at[2, pl.ds(0, last), :, my_rows, :], t_send.at[1, k - 1], t_recv.at[0, 0, k - 1], beside
        ).wait_send()
        t_rows(2, last, k, my_col, own_side).wait_send()


def local(coefficients, transfer):
    cols = lax.axis_size("col")
    nodes_here, rank, columns = coefficients.shape
    levels, _, children, rows, _ = transfer.shape
    width = min(WIDTH, columns)
    chunks = columns // width
    units = nodes_here * chunks
    plain = units - chunks
    others = max(cols - 1, 1)
    kind = coefficients.dtype
    block = (rank, width)
    dma = pltpu.SemaphoreType.DMA
    return pl.pallas_call(
        functools.partial(kernel, cols, chunks),
        out_shape=pltpu.VMEM(coefficients.shape, kind),
        in_specs=[pl.BlockSpec(memory_space=pl.ANY)] * 2,
        out_specs=pl.BlockSpec(memory_space=pltpu.VMEM),
        scratch_shapes=[
            pltpu.VMEM(coefficients.shape, kind),
            pltpu.VMEM((levels, nodes_here, children, rank, rank), kind),
            pltpu.VMEM((nodes_here, children - 1, rank, rank), kind),
            pltpu.VMEM((2, rows, rank), kind),
            pltpu.VMEM((2, 2, rank, rank), kind),
            pltpu.VMEM((units, 2) + block, kind),
            pltpu.VMEM((units, 2) + block, kind),
            pltpu.VMEM((units,) + block, kind),
            pltpu.VMEM((units,) + block, kind),
            pltpu.VMEM((units, 2) + block, kind),
            pltpu.VMEM((units,) + block, kind),
            pltpu.VMEM((units,) + block, kind),
            pltpu.VMEM((2, chunks) + block, kind),
            dma((2,)),
            dma((8,)),
            dma((4, units)),
            dma((chunks,)),
            dma((2, others)),
            dma((2,)),
            dma((3, others)),
            dma((levels, nodes_here, others)),
            dma((2,)),
            dma((nodes_here,)),
            dma((2,)),
            dma((3,)),
            dma((others,)),
            dma((others,)),
        ],
        compiler_params=pltpu.CompilerParams(
            collective_id=0, has_side_effects=True, vmem_limit_bytes=56 * 1024 * 1024
        ),
    )(coefficients, transfer)


def solution(mesh):
    return jax.shard_map(
        local,
        mesh=mesh,
        in_specs=(P("node", None, "col"), P(None, "node", None, "col", None)),
        out_specs=P("node", None, "col"),
        check_vma=False,
    )
```

```python
import functools

import jax
import jax.numpy as jnp
from jax import lax
from jax.experimental import pallas as pl
from jax.experimental.pallas import tpu as pltpu
from jax.sharding import PartitionSpec as P

MESH = pl.DeviceIdType.MESH
WIDTH = 256
HELD_BACK = 4
LAG_ONE, LAG_RELAY, LAG_FAR, LAG_MID, LAG_NEAR, LAG_END = 2, 4, 5, 7, 11, 10
TO_TWO, FORWARD, TO_PAIR, TO_ACROSS, RELAY, PARTIAL, SUM_NEAR, SUM_FAR = range(8)
ROW = {TO_TWO: 0, FORWARD: 1, TO_PAIR: 2, TO_ACROSS: 3, RELAY: 3, PARTIAL: 3, SUM_NEAR: 3, SUM_FAR: 3}


def flip(i, bit):
    return i + bit - 2 * bit * (i // bit % 2)


def dot(a, b):
    return jnp.dot(a, b, preferred_element_type=jnp.float32)


def kernel(
    cols, chunks, x_in, t_in, out_ref,
    x, t, t_far, t_pass, t_sum, held, theirs, y1, pair, come, partial_out, partial_in, sums,
    local_sem, send, recv, far_sum, half_x, half_core, t_send, t_recv, far_send, far_recv, sum_send, sum_recv, spread_send, spread_recv,
):
    nodes_here = x_in.shape[0]
    last = nodes_here - 1
    rows = t_in.shape[3]
    units = nodes_here * chunks
    plain = last * chunks
    width = x_in.shape[2] // chunks
    me = lax.axis_index("node")
    my_col = lax.axis_index("col")
    one = me % 4
    two = me // 4 % 4
    side = two // 2 * 2
    other = 2 - side
    is_mid = (two + 1) // 2 % 2 == 1
    is_end = (two + 1) // 2 % 2 == 0
    by_core, by_two, by_pair = flip(me, 1), flip(me, 2), flip(me, 4)
    by_across = flip(by_pair, 8)
    my_rows = pl.ds(my_col * rows, rows)

    barrier = pltpu.get_barrier_semaphore()
    for k in range(1, cols):
        pl.semaphore_signal(barrier, inc=1, device_id={"col": (my_col + k) % cols}, device_id_type=MESH)
    for device in (by_pair, by_two, by_core):
        pl.semaphore_signal(barrier, inc=1, device_id={"node": device}, device_id_type=MESH)

    @pl.when(is_mid)
    def _():
        pl.semaphore_signal(barrier, inc=1, device_id={"node": by_across}, device_id_type=MESH)

    x_copy = pltpu.make_async_copy(x_in, x, local_sem.at[0])
    x_copy.start()
    t_copy = pltpu.make_async_copy(t_in, t.at[:, :, :, my_rows, :], local_sem.at[1])
    t_copy.start()

    @pl.when(is_mid)
    def _():
        pl.semaphore_wait(barrier, 4 + cols - 1)

    @pl.when(is_end)
    def _():
        pl.semaphore_wait(barrier, 3 + cols - 1)

    def remote(source, target, send_sem, recv_sem, device):
        return pltpu.make_async_remote_copy(
            src_ref=source, dst_ref=target, send_sem=send_sem, recv_sem=recv_sem,
            device_id=device, device_id_type=MESH,
        )

    def t_rows(level, m, k, col, children=None):
        here = pl.ds(col * rows, rows)
        if children is None:
            source, target = t_in.at[level, m], t.at[level, m, :, here, :]
        else:
            source, target = t_in.at[level, m, children], t.at[level, m, children, here, :]
        group = 0 if level < 2 else 1 if children is None else 2
        return remote(
            source, target, t_send.at[group, k - 1], t_recv.at[level, m, k - 1], {"col": (my_col + k) % cols}
        )

    def wait_rows(level, m, children=None):
        for k in range(1, cols):
            t_rows(level, m, k, (my_col + cols - k) % cols, children).wait_recv()

    own_side = pl.ds(side, 2)

    order = sorted(
        (3 * m + 2 * level, level, m) for m in range(nodes_here) for level in range(3) if (level, m) != (2, last)
    )
    for _, level, m in order:
        for k in range(1, cols):
            t_rows(level, m, k, my_col).start()

    given = t_in.at[2, last, pl.ds(other, 2)]

    def give():
        return remote(given, t_sum.at[0, :, my_rows, :], sum_send.at[0], sum_recv.at[0], {"node": by_across})

    def give_pair():
        return remote(given, t_pass, sum_send.at[0], sum_recv.at[2], {"node": by_pair})

    def give_on():
        return remote(t_pass, t_sum.at[1, :, my_rows, :], sum_send.at[1], sum_recv.at[1], {"node": by_across})

    @pl.when(is_mid)
    def _():
        give().start()

    @pl.when(is_end)
    def _():
        give_pair().start()

    def spread(k, col):
        part = t_sum.at[:, :, pl.ds(col * rows, rows), :]
        return remote(part, part, spread_send.at[k - 1], spread_recv.at[k - 1], {"col": (my_col + k) % cols})

    def copy(kind, u):
        source, target, device = {
            TO_TWO: lambda: (held.at[u, 0], held.at[u, 1], by_two),
            FORWARD: lambda: (held.at[u], theirs.at[u], by_core),
            TO_PAIR: lambda: (y1.at[u], pair.at[u], by_pair),
            TO_ACROSS: lambda: (y1.at[u], come.at[u, 0], by_across),
            RELAY: lambda: (pair.at[u], come.at[u, 1], by_across),
            PARTIAL: lambda: (partial_out.at[u], partial_in.at[u], by_pair),
            SUM_NEAR: lambda: (sums.at[0, u - plain], come.at[u, 0], by_across),
            SUM_FAR: lambda: (sums.at[1, u - plain], come.at[u, 1], by_across),
        }[kind]()
        sem = far_sum.at[u - plain] if kind == SUM_FAR else recv.at[ROW[kind], u]
        return remote(source, target, send.at[kind], sem, {"node": device})

    def sent(kind, source, target):
        remote(source, target, send.at[kind], recv.at[ROW[kind], 0], {"node": by_pair}).wait_send()

    def far(m):
        if isinstance(m, int) and m == last:
            source, target, sem = t.at[2, m, flip(two, 1)], t_far.at[m, 0], far_send.at[1]
        else:
            source, target, sem = t.at[2, m, pl.ds(1 - two // 3, 3)], t_far.at[m], far_send.at[0]
        return remote(source, target, sem, far_recv.at[m], {"node": by_pair})

    def store(u, total):
        columns = pl.ds(pl.multiple_of(u % chunks * width, width), width)
        out_ref[u // chunks, :, columns] = total.astype(out_ref.dtype)

    def first(u, action):
        @pl.when(u % chunks == 0)
        def _():
            action(u // chunks)

    def all_columns(u):
        return pl.ds(pl.multiple_of(u % chunks * width, width), width)

    def piece_to_two(u, here, columns, sem):
        return remote(held.at[u, 0, here, columns], held.at[u, 1, here, columns], send.at[TO_TWO], sem, {"node": by_two})

    def zero_rows(u, here, wanted, columns, sem):
        total = dot(t[0, 0, 0, here], x[0, :, wanted])
        for j in range(1, 4):
            total += dot(t[0, 0, j, here], x[j, :, wanted])
        held[u, 0, here, columns] = total.astype(held.dtype)
        piece_to_two(u, here, columns, sem).start()

    def rows_of(k):
        return pl.ds(pl.multiple_of((my_col + k) % cols * rows, rows), rows)

    whole = pl.ds(0, width)

    def own_rows(u, _):
        zero_rows(u, rows_of(0), all_columns(u), whole, recv.at[ROW[TO_TWO], u])
        return 0

    def other_rows(u, _):
        for k in range(1, cols):
            zero_rows(u, rows_of(k), all_columns(u), whole, recv.at[ROW[TO_TWO], u])
        return 0

    halves = [pl.ds(h * width // 2, width // 2) for h in range(2)]

    def half_to_core(h):
        source, target = held.at[0, :, :, halves[h]], theirs.at[0, :, :, halves[h]]
        return remote(source, target, send.at[FORWARD], half_core.at[h], {"node": by_core})

    def one_rows(here, columns):
        total = dot(t[1, 0, one, here], held[0, 0, :, columns])
        total += dot(t[1, 0, flip(one, 2), here], held[0, 1, :, columns])
        total += dot(t[1, 0, flip(one, 1), here], theirs[0, 0, :, columns])
        total += dot(t[1, 0, 3 - one, here], theirs[0, 1, :, columns])
        y1[0, here, columns] = total.astype(y1.dtype)

        def part(kind, target, device):
            remote(
                y1.at[0, here, columns], target.at[here, columns],
                send.at[kind], recv.at[ROW[kind], 0], {"node": device},
            ).start()

        pl.when(is_mid)(lambda: part(TO_ACROSS, come.at[0, 0], by_across))
        pl.when(is_end)(lambda: part(TO_PAIR, pair.at[0], by_pair))

    def forward(u):
        copy(TO_TWO, u).wait_recv()
        copy(FORWARD, u).start()

    def first_unit():
        wait_rows(0, 0)
        for h in range(2):
            for k in range(1, cols):
                zero_rows(0, rows_of(k), halves[h], halves[h], half_x.at[h, k - 1])
        lax.fori_loop(1, chunks, other_rows, 0)
        piece_to_two(0, rows_of(0), whole, recv.at[ROW[TO_TWO], 0]).wait_recv()
        for h in range(2):
            for k in range(1, cols):
                piece_to_two(0, rows_of(k), halves[h], half_x.at[h, k - 1]).wait_recv()
            half_to_core(h).start()
        for h in range(2):
            half_to_core(h).wait_recv()
            one_rows(rows_of(0), halves[h])
        if chunks > 1:
            forward(1)
        wait_rows(1, 0)
        for k in range(1, cols):
            one_rows(rows_of(k), whole)

    def stage_zero(u):
        first(u, lambda m: wait_rows(0, m))
        m = u // chunks
        columns = all_columns(u)
        total = dot(t[0, m, 0], x[0, :, columns])
        for j in range(1, 4):
            total += dot(t[0, m, j], x[j, :, columns])
        held[u, 0] = total.astype(held.dtype)
        copy(TO_TWO, u).start()

    def stage_one(u):
        pl.when(u > (1 if chunks > 1 else 0))(lambda: forward(u))
        first(u, lambda m: wait_rows(1, m))
        m = u // chunks
        total = dot(t[1, m, one], held[u, 0])
        total += dot(t[1, m, flip(one, 2)], held[u, 1])
        copy(FORWARD, u).wait_recv()
        total += dot(t[1, m, flip(one, 1)], theirs[u, 0])
        total += dot(t[1, m, 3 - one], theirs[u, 1])
        y1[u] = total.astype(y1.dtype)

        @pl.when(is_mid & (u < plain))
        def _():
            copy(TO_ACROSS, u).start()

        @pl.when(is_end)
        def _():
            copy(TO_PAIR, u).start()

    def stage_relay(u):
        copy(TO_PAIR, u).wait_recv()

        @pl.when(u < plain)
        def _():
            copy(RELAY, u).start()

        @pl.when(u >= plain)
        def _():
            @pl.when(u == plain)
            def _():
                for k in range(1, cols):
                    spread(k, (my_col + cols - k) % cols).wait_recv()

            for who, kind in ((1, SUM_FAR), (0, SUM_NEAR)):
                total = dot(t_sum[who, two % 2], y1[u]) + dot(t_sum[who, 1 - two % 2], pair[u])
                sums[who, u - plain] = total.astype(sums.dtype)
                if kind == SUM_FAR:
                    copy(kind, u).start()

            @pl.when(u < units - HELD_BACK)
            def _():
                copy(SUM_NEAR, u).start()

            @pl.when(u == units - 1)
            def _():
                for late in range(min(HELD_BACK, chunks), 0, -1):
                    copy(SUM_NEAR, units - late).start()

    def stage_far(m):
        wait_rows(2, m, own_side if m == last else None)
        far(m).start()

    def own_part(u):
        m = u // chunks
        return dot(t[2, m, two], y1[u])

    def pair_part(u):
        return dot(t[2, u // chunks, flip(two, 1)], pair[u])

    def stage_mid(u):
        @pl.when(u < plain)
        def _():
            def arrive(m):
                wait_rows(2, m)
                far(m).wait_recv()

            first(u, arrive)
            m = u // chunks
            remote(come.at[u], come.at[u], send.at[RELAY], recv.at[ROW[RELAY], u], {"node": by_across}).wait_recv()
            start = 1 - two // 2
            part = dot(t_far[m, 3 - two - start], come[u, 0])
            part += dot(t_far[m, flip(3 - two, 1) - start], come[u, 1])
            part += dot(t_far[m, two - start], y1[u])
            partial_out[u] = part.astype(partial_out.dtype)
            copy(PARTIAL, u).start()
            total = own_part(u) + pair_part(u)
            total += dot(t[2, m, 3 - two], come[u, 0])
            total += dot(t[2, m, flip(two, 2)], come[u, 1])
            store(u, total)

        @pl.when(u >= plain)
        def _():
            @pl.when(u == plain)
            def _():
                wait_rows(2, last, own_side)
                far(last).wait_recv()

            copy(SUM_FAR, u).wait_recv()
            part = dot(t_far[last, 0], y1[u]) + come[u, 1].astype(jnp.float32)
            partial_out[u] = part.astype(partial_out.dtype)
            copy(PARTIAL, u).start()

    def stage_near(u):
        @pl.when(u >= plain)
        def _():
            total = own_part(u) + pair_part(u)
            copy(SUM_NEAR, u).wait_recv()
            store(u, total + come[u, 0].astype(jnp.float32))

    def stage_end(u):
        total = own_part(u)
        copy(PARTIAL, u).wait_recv()
        store(u, total + partial_in[u].astype(jnp.float32))

    x_copy.wait()
    t_copy.wait()
    lax.fori_loop(0, chunks, own_rows, 0)

    @pl.when(is_mid)
    def _():
        give_pair().wait_recv()
        give_on().start()

    first_unit()

    def step(s, _):
        def run(stage, lag, role=None, start=0):
            u = s - lag
            ready = (u >= start) & (u < units)

            @pl.when(ready if role is None else ready & role)
            def _():
                stage(u)

        run(stage_relay, LAG_RELAY, is_mid)
        run(stage_mid, LAG_MID, is_mid)
        run(stage_near, LAG_NEAR, is_mid)
        run(stage_one, LAG_ONE, start=1)
        @pl.when(s == LAG_ONE + 1)
        def _():
            @pl.when(is_mid)
            def _():
                give().wait_recv()
                give_on().wait_recv()
                for k in range(1, cols):
                    spread(k, my_col).start()

            for k in range(1, cols):
                t_rows(2, last, k, my_col, own_side).start()

        run(stage_zero, 0, start=chunks)
        for m in range(nodes_here):

            @pl.when(is_end & (s == LAG_FAR + m * chunks))
            def _(m=m):
                stage_far(m)

        run(stage_end, LAG_END, is_end)
        return 0

    lax.fori_loop(LAG_ONE + 1, units + max(LAG_NEAR, LAG_END), step, 0)

    sent(TO_TWO, held.at[:, 0], held.at[:, 1])
    sent(FORWARD, held, theirs)

    @pl.when(is_mid)
    def _():
        early = pl.ds(0, plain)
        late = pl.ds(plain, units - plain)
        sent(TO_ACROSS, y1.at[early], come.at[early, 0])
        sent(RELAY, pair.at[early], come.at[early, 1])
        sent(PARTIAL, partial_out, partial_in)
        sent(SUM_NEAR, sums.at[0], come.at[late, 0])
        sent(SUM_FAR, sums.at[1], come.at[late, 0])
        give().wait_send()
        give_on().wait_send()
        for k in range(1, cols):
            spread(k, my_col).wait_send()

    @pl.when(is_end)
    def _():
        sent(TO_PAIR, y1, pair)
        full = t_far.at[pl.ds(0, last)]
        remote(full, full, far_send.at[0], far_recv.at[0], {"node": by_pair}).wait_send()
        far(last).wait_send()
        give_pair().wait_send()

    for k in range(1, cols):
        beside = {"col": (my_col + k) % cols}
        both, rest = t_in.at[pl.ds(0, 2)], t_in.at[2, pl.ds(0, last)]
        remote(both, t.at[pl.ds(0, 2), :, :, my_rows, :], t_send.at[0, k - 1], t_recv.at[0, 0, k - 1], beside).wait_send()
        remote(
            rest, t.at[2, pl.ds(0, last), :, my_rows, :], t_send.at[1, k - 1], t_recv.at[0, 0, k - 1], beside
        ).wait_send()
        t_rows(2, last, k, my_col, own_side).wait_send()


def local(coefficients, transfer):
    cols = lax.axis_size("col")
    nodes_here, rank, columns = coefficients.shape
    levels, _, children, rows, _ = transfer.shape
    width = min(WIDTH, columns)
    chunks = columns // width
    units = nodes_here * chunks
    plain = units - chunks
    others = max(cols - 1, 1)
    kind = coefficients.dtype
    block = (rank, width)
    dma = pltpu.SemaphoreType.DMA
    return pl.pallas_call(
        functools.partial(kernel, cols, chunks),
        out_shape=pltpu.VMEM(coefficients.shape, kind),
        in_specs=[pl.BlockSpec(memory_space=pl.ANY)] * 2,
        out_specs=pl.BlockSpec(memory_space=pltpu.VMEM),
        scratch_shapes=[
            pltpu.VMEM(coefficients.shape, kind),
            pltpu.VMEM((levels, nodes_here, children, rank, rank), kind),
            pltpu.VMEM((nodes_here, children - 1, rank, rank), kind),
            pltpu.VMEM((2, rows, rank), kind),
            pltpu.VMEM((2, 2, rank, rank), kind),
            pltpu.VMEM((units, 2) + block, kind),
            pltpu.VMEM((units, 2) + block, kind),
            pltpu.VMEM((units,) + block, kind),
            pltpu.VMEM((units,) + block, kind),
            pltpu.VMEM((units, 2) + block, kind),
            pltpu.VMEM((units,) + block, kind),
            pltpu.VMEM((units,) + block, kind),
            pltpu.VMEM((2, chunks) + block, kind),
            dma((2,)),
            dma((8,)),
            dma((4, units)),
            dma((chunks,)),
            dma((2, others)),
            dma((2,)),
            dma((3, others)),
            dma((levels, nodes_here, others)),
            dma((2,)),
            dma((nodes_here,)),
            dma((2,)),
            dma((3,)),
            dma((others,)),
            dma((others,)),
        ],
        compiler_params=pltpu.CompilerParams(
            collective_id=0, has_side_effects=True, vmem_limit_bytes=56 * 1024 * 1024
        ),
    )(coefficients, transfer)


def solution(mesh):
    return jax.shard_map(
        local,
        mesh=mesh,
        in_specs=(P("node", None, "col"), P(None, "node", None, "col", None)),
        out_specs=P("node", None, "col"),
        check_vma=False,
    )
```
